512 devices in a mesh: rep: 32 (over x_lo, z, core), shard: 16 (over y, x_hi).
Axes of the slice: x: 4 (x_hi: 2, x_lo: 2; x = x_hi * 2 + x_lo), y: 8, z: 8, core: 2. Of those that a mesh axis runs over, the one named last changes fastest.
Arguments:
- outer_delta: float32 [32, 4194304], P('rep', 'shard'), may hold values from -40 to 40
- offsets: int32 [65], replicated, may hold values from 0 to 4194304, as said below
- parameters: float32 [4194304], P('shard'), may hold values from -6 to 6
- momentum: float32 [4194304], P(('shard', 'rep')), may hold values from -1.2 to 1.2
Outputs:
- new_parameters: float32 [4194304], P('shard')
- new_momentum: float32 [4194304], P(('shard', 'rep'))
The draws below stay inside these ranges and needn't reach their ends.
Inputs may be any that keep to these rules, and one draw needn't show every extreme that they name: `offsets`: strictly increasing multiples of 128, the first 0 and the last 4194304.
All inputs are finite; a program needn't handle non-finite values.
Results may differ from the reference program's by a relative error of at most 0.0003.
Values sent between devices are 32-bit elements; how exact they have to be, the bound alone decides.
A program may use at most 64 MiB of HBM per device.

```python
import jax
import jax.numpy as jnp
from jax import lax

TENSORS = 64
PARAMS = 4194304
REPLICAS = 32


def tensor_bounds(key):
    slots = PARAMS // 128
    shuffled = jax.random.permutation(jax.random.fold_in(key, 11), slots - 1) + 1
    inner = jnp.sort(shuffled[:TENSORS - 1]) * 128
    first = jnp.zeros((1,), jnp.int32)
    final = jnp.full((1,), PARAMS, jnp.int32)
    return jnp.concatenate([first, inner.astype(jnp.int32), final]).astype(jnp.int32)


def draw_offsets(key, part):
    return tensor_bounds(key)


def draw_outer_delta(key, part):
    bounds = tensor_bounds(key)
    positions = jnp.arange(PARAMS, dtype=jnp.int32)
    segment = jnp.searchsorted(bounds, positions, side='right') - 1
    log_scale = jax.random.uniform(jax.random.fold_in(key, 12), (TENSORS,), jnp.float32, jnp.log(0.05), jnp.log(0.5))
    tensor_scale = jnp.exp(log_scale)
    ramp = 1.0 + 2.0 * positions.astype(jnp.float32) / PARAMS
    rep_scale = 1.0 + 2.0 * jnp.arange(REPLICAS, dtype=jnp.float32) / max(REPLICAS - 1, 1)
    noise = jnp.clip(jax.random.normal(jax.random.fold_in(key, 13), (REPLICAS, PARAMS), jnp.float32), -5.0, 5.0)
    return (noise * rep_scale[:, None] * (tensor_scale[segment] * ramp)[None, :]).astype(jnp.float32)


def steps_of(stream_key, shape, pieces, smallest, high):
    factor_of, own = 1.0, jax.random.fold_in(stream_key, 6)
    for axis_at, blocks in pieces:
        heights = jnp.exp(jax.random.uniform(jax.random.fold_in(own, axis_at), (blocks,), jnp.float32, smallest / len(pieces), high / len(pieces)))
        factor_of = factor_of * jnp.repeat(heights, shape[axis_at] // blocks).reshape([-1 if axis == axis_at else 1 for axis in range(len(shape))])
    return factor_of


def bell_draw(key, dims, scale, most, shards=(), kind=jnp.bfloat16):
    result = jax.random.normal(key, dims, jnp.float32) * scale
    if len(shards) > 0:
        result = steps_of(key, dims, shards, -0.22, 0.18) * result
    return jnp.clip(result, min=-most, max=most).astype(kind)


def setup_inputs(seed: int = 0) -> dict:
    streams_of = jax.random.split(jax.random.key(seed), 5)
    return {
        "outer_delta": draw_outer_delta(jax.random.fold_in(streams_of[4], 71), 0),
        "offsets": draw_offsets(jax.random.fold_in(streams_of[4], 71), 0),
        "parameters": bell_draw(streams_of[2], (PARAMS,), 1.0, 6.0, ((0, 16),), jnp.float32),
        "momentum": bell_draw(streams_of[3], (PARAMS,), 0.2, 1.2, ((0, 512),), jnp.float32),
    }


LR_OUTER = 0.7
MU_OUTER = 0.9
CLIP_RMS = 0.1
EPSILON = 1e-06

def reference(outer_delta, offsets, parameters, momentum):
    avg_delta = lax.optimization_barrier(jnp.sum(outer_delta, axis=0)) / jnp.float32(REPLICAS)
    positions = jnp.arange(PARAMS, dtype=jnp.int32)
    segment = (jnp.searchsorted(offsets, positions, side='right') - 1).astype(jnp.int32)
    squares_sum = jax.ops.segment_sum(avg_delta * avg_delta, segment, num_segments=TENSORS)
    lengths = (offsets[1:] - offsets[:-1]).astype(jnp.float32)
    factor = jnp.minimum(1.0, CLIP_RMS * jnp.sqrt(lengths) * lax.rsqrt(squares_sum + EPSILON))
    scaled = avg_delta * factor[segment]
    new_momentum = MU_OUTER * momentum + scaled
    new_parameters = parameters - LR_OUTER * (scaled + MU_OUTER * new_momentum)
    return (new_parameters, new_momentum)
```

```python
import functools

import jax
import jax.numpy as jnp
from jax import lax
from jax.experimental import pallas as pl
from jax.experimental.pallas import tpu as pltpu
from jax.sharding import Mesh
from jax.sharding import PartitionSpec as P

X, Z, CORE, Y, XH = "rep_0", "rep_1", "rep_2", "shard_0", "shard_1"
AXES = (X, Z, CORE, Y, XH)
REP = (X, Z, CORE)
SHARD = (Y, XH)
SHARD_REP = (Y, XH, X, Z, CORE)

LR_OUTER = 0.7
MU_OUTER = 0.9
CLIP_RMS = 0.1
EPSILON = 1e-06


def remote(src, dst, send, recv, dev):
    return pltpu.make_async_remote_copy(
        src_ref=src,
        dst_ref=dst,
        send_sem=send,
        recv_sem=recv,
        device_id=dev,
        device_id_type=pl.DeviceIdType.MESH,
    )


def far_first(n):
    order = [n // 2] if n % 2 == 0 else []
    for d in range((n - 1) // 2, 0, -1):
        order += [d, n - d]
    return order


def step_kernel(
    sizes,
    delta, mom, par, offs,
    newp, newm,
    dl, sib, xs, xr, zs, zr, ga, gm, pv, ov, sqy, sqx, sqz,
    lsem, rs_core, rs_x, rs_z, ag_z, ag_x, ag_core, m_z, m_x, m_core, qy, qx, qz,
):
    nx, nz, nc, ny, nh = (sizes[a] for a in AXES)
    x, z, c, y, h = (lax.axis_index(a) for a in AXES)
    rows = xs.shape[1]
    x_nb, c_nb = {X: 1 - x}, {CORE: 1 - c}
    zof = lambda d: lax.rem(z + d + nz, nz)
    order = far_first(nz)
    nd = len(order)
    mine = x * nz + z

    barrier = pltpu.get_barrier_semaphore()
    z_peers = [{Z: zof(d)} for d in order]
    y_peers = [{Y: lax.rem(y + d, ny)} for d in range(1, ny)]
    x_peers = [
        {XH: lax.rem(h + a, nh), X: lax.rem(x + b, nx), CORE: lax.rem(c + e, nc)}
        for a in range(nh) for b in range(nx) for e in range(nc) if a or b or e
    ]
    peers = z_peers + y_peers + x_peers
    for dev in peers:
        pl.semaphore_signal(barrier, inc=1, device_id=dev, device_id_type=pl.DeviceIdType.MESH)

    load_m = pltpu.make_async_copy(mom, gm.at[mine, c], lsem.at[0])
    load_m.start()
    load_away = pltpu.make_async_copy(delta.at[:, pl.ds(1 - c, 1)], dl.at[:, pl.ds(1 - c, 1)], lsem.at[1])
    load_away.start()
    load_own = pltpu.make_async_copy(delta.at[:, pl.ds(c, 1)], dl.at[:, pl.ds(c, 1)], lsem.at[2])
    load_own.start()
    load_o = pltpu.make_async_copy(offs, ov, lsem.at[3])
    load_o.start()
    load_p = pltpu.make_async_copy(par, pv, lsem.at[4])
    load_p.start()

    load_m.wait()
    load_away.wait()
    pl.semaphore_wait(barrier, len(peers))

    pending = []

    def send(src, dst, sems, i, dev):
        copy = remote(src, dst, sems.at[0, i], sems.at[1, i], dev)
        copy.start()
        pending.append(copy)

    def wait_in(dst, sems, i, dev):
        remote(dst, dst, sems.at[0, i], sems.at[1, i], dev).wait_recv()

    steps = order + [0]
    q_of = lambda xx, i: xx * nz + zof(steps[i])

    for i in range(nz):
        q = q_of(1 - x, i)
        send(dl.at[q, 1 - c], sib.at[q], rs_core, i, c_nb)
    for i in range(nz):
        q = q_of(x, i)
        send(dl.at[q, 1 - c], sib.at[q], rs_core, nz + i, c_nb)

    s = 1 - 2 * c
    na, nb = nz // 2, nz - 1 - nz // 2
    fwd, bwd = {Z: zof(s)}, {Z: zof(-s)}
    origin_a = lambda k: x * nz + zof(-s * k)
    origin_b = lambda k: x * nz + zof(s * k)
    send(gm.at[mine, c], gm.at[mine, c], m_z, 0, fwd)
    send(gm.at[mine, c], gm.at[mine, c], m_z, na, bwd)
    send(gm.at[mine, c], gm.at[mine, c], m_x, 0, x_nb)
    send(gm.at[mine, c], gm.at[mine, c], m_core, 0, c_nb)

    def momentum_step(k):
        if k <= na:
            blk = gm.at[origin_a(k), c]
            wait_in(blk, m_z, k - 1, fwd)
            if k < na:
                send(blk, blk, m_z, k, fwd)
            send(blk, blk, m_x, k, x_nb)
            send(blk, blk, m_core, k, c_nb)
        if k <= nb:
            blk = gm.at[origin_b(k), c]
            wait_in(blk, m_z, na + k - 1, bwd)
            if k < nb:
                send(blk, blk, m_z, na + k, bwd)
            send(blk, blk, m_x, na + k, x_nb)
            send(blk, blk, m_core, na + k, c_nb)

    load_own.wait()

    for i in range(nz):
        q = q_of(1 - x, i)
        wait_in(sib.at[q], rs_core, i, c_nb)
        xs[i] = dl[q, c] + sib[q]
        send(xs.at[i], xr.at[i], rs_x, i, x_nb)

    momentum_step(1)

    for i in range(nz):
        q = q_of(x, i)
        wait_in(sib.at[q], rs_core, nz + i, c_nb)
        part = dl[q, c] + sib[q]
        wait_in(xr.at[i], rs_x, i, x_nb)
        zs[i] = part + xr[i]
        if i < nd:
            send(zs.at[i], zr.at[i], rs_z, i, {Z: zof(steps[i])})
        if i == nz // 2 - 1:
            momentum_step(2)
        if i == nz - 2:
            momentum_step(3)

    total = zs[nz - 1]
    for i in range(nd):
        wait_in(zr.at[i], rs_z, i, z_peers[i])
        total = total + zr[i]
    avg = total * (1.0 / (nx * nz * nc))
    ga[mine, c] = avg

    load_o.wait()
    low = ov[:, 0 : ov.shape[1] - 1]
    high = ov[:, 1 : ov.shape[1]]
    own_len = rows * 128
    shard_pos = (y * nh + h) * (nx * nz * nc * own_len)

    def row_mask(first_pos):
        pos = first_pos + 128 * lax.broadcasted_iota(jnp.int32, (rows, low.shape[1]), 0)
        return (pos >= low) & (pos < high)

    squares = jnp.sum(avg * avg, axis=1, keepdims=True)
    mask = row_mask(shard_pos + (mine * nc + c) * own_len)
    sqy[y] = jnp.sum(jnp.where(mask, squares, 0.0), axis=0, keepdims=True)
    for i, dev in enumerate(y_peers):
        send(sqy.at[y], sqy.at[y], qy, i, dev)

    for i in range(nd):
        send(ga.at[mine, c], ga.at[mine, c], ag_z, i, z_peers[i])
    send(ga.at[mine, c], ga.at[mine, c], ag_x, nd, x_nb)
    send(ga.at[mine, c], ga.at[mine, c], ag_core, nd, c_nb)

    def mean_from_z(i):
        blk = ga.at[x * nz + zof(-steps[i]), c]
        wait_in(blk, ag_z, i, z_peers[i])
        send(blk, blk, ag_x, i, x_nb)
        send(blk, blk, ag_core, i, c_nb)

    def mean_from_x(i):
        blk = ga.at[(1 - x) * nz + zof(-steps[i]), c]
        wait_in(blk, ag_x, i, x_nb)
        send(blk, blk, ag_core, nz + i, c_nb)

    def m_slot(xx, j):
        return xx * nz + (zof(-s * j) if j <= na else zof(s * (j - na)))

    momentum_step(4) if na >= 4 else None
    for j in range(nz):
        blk = gm.at[m_slot(1 - x, j), c]
        wait_in(blk, m_x, j, x_nb)
        send(blk, blk, m_core, nz + j, c_nb)

    for i in range(ny - 1):
        src = lax.rem(y + ny - 1 - i, ny)
        wait_in(sqy.at[src], qy, i, y_peers[i])
    acc = sqy[0]
    for i in range(1, ny):
        acc = acc + sqy[i]
    slot = (h * nx + x) * nc + c
    sqx[slot] = acc
    for i, dev in enumerate(x_peers):
        send(sqx.at[slot], sqx.at[slot], qx, i, dev)

    for i in range(nd):
        mean_from_z(i)

    i = 0
    for a in range(nh):
        for b in range(nx):
            for e in range(nc):
                if a or b or e:
                    hh, xx, cc = lax.rem(h + nh - a, nh), lax.rem(x + nx - b, nx), lax.rem(c + nc - e, nc)
                    wait_in(sqx.at[(hh * nx + xx) * nc + cc], qx, i, x_peers[i])
                    i += 1
    acc = sqx[0]
    for i in range(1, nh * nx * nc):
        acc = acc + sqx[i]
    sqz[z] = acc
    for i in range(nd):
        send(sqz.at[z], sqz.at[z], qz, i, z_peers[i])

    mean_from_x(nd)
    for i in range(nd):
        mean_from_x(i)

    for i in range(nd):
        wait_in(sqz.at[zof(-steps[i])], qz, i, z_peers[i])
    acc = sqz[0]
    for i in range(1, nz):
        acc = acc + sqz[i]
    lengths = (high - low).astype(jnp.float32)
    factor = jnp.minimum(1.0, CLIP_RMS * jnp.sqrt(lengths) * lax.rsqrt(acc + EPSILON))

    for i in range(nz):
        for g, xx in ((0, x), (1, 1 - x)):
            wait_in(ga.at[xx * nz + zof(-steps[i]), 1 - c], ag_core, g * nz + i, c_nb)
    other = -s
    for j in range(nz):
        for g, xx in ((0, x), (1, 1 - x)):
            zz = zof(-other * j) if j <= na else zof(other * (j - na))
            wait_in(gm.at[xx * nz + zz, 1 - c], m_core, g * nz + j, c_nb)

    load_p.wait()
    for copy in pending:
        copy.wait_send()

    def apply(b, carry):
        q, cc = b // nc, lax.rem(b, nc)
        m = row_mask(shard_pos + b * own_len)
        row_factor = jnp.sum(jnp.where(m, factor, 0.0), axis=1, keepdims=True)
        scaled = ga[q, cc] * row_factor
        momentum = MU_OUTER * gm[q, cc] + scaled
        newp[q, cc] = pv[q, cc] - LR_OUTER * (scaled + MU_OUTER * momentum)
        return carry

    lax.fori_loop(0, nx * nz * nc, apply, 0)
    m = row_mask(shard_pos + (mine * nc + c) * own_len)
    row_factor = jnp.sum(jnp.where(m, factor, 0.0), axis=1, keepdims=True)
    newm[...] = MU_OUTER * gm[mine, c] + ga[mine, c] * row_factor


def on_device(sizes, outer_delta, offsets, parameters, momentum):
    nx, nz, nc, ny, nh = (sizes[a] for a in AXES)
    rows = momentum.shape[0] // 128
    nq = nx * nz
    whole = (nq, nc, rows, 128)
    block = (rows, 128)
    f32 = jnp.float32
    dma = lambda n: pltpu.SemaphoreType.DMA((2, n))
    vmem = pltpu.VMEM
    tensors = offsets.shape[0] - 1
    new_parameters, new_momentum = pl.pallas_call(
        functools.partial(step_kernel, sizes),
        out_shape=(jax.ShapeDtypeStruct(whole, f32), jax.ShapeDtypeStruct(block, f32)),
        in_specs=[pl.BlockSpec(memory_space=pl.ANY)] * 4,
        out_specs=(pl.BlockSpec(memory_space=pltpu.VMEM),) * 2,
        scratch_shapes=[
            vmem(whole, f32),
            vmem((nq,) + block, f32),
            vmem((nz,) + block, f32),
            vmem((nz,) + block, f32),
            vmem((nz,) + block, f32),
            vmem((nz,) + block, f32),
            vmem(whole, f32),
            vmem(whole, f32),
            vmem(whole, f32),
            vmem((1, tensors + 1), jnp.int32),
            vmem((ny, 1, tensors), f32),
            vmem((nh * nx * nc, 1, tensors), f32),
            vmem((nz, 1, tensors), f32),
            pltpu.SemaphoreType.DMA((5,)),
            dma(nq), dma(nz), dma(nz), dma(nz), dma(nz), dma(nq), dma(nz), dma(nz), dma(nq),
            dma(ny), dma(nh * nx * nc), dma(nz),
        ],
        compiler_params=pltpu.CompilerParams(
            collective_id=0, has_side_effects=True, vmem_limit_bytes=24 * 1024 * 1024
        ),
    )(
        outer_delta.reshape(whole),
        momentum.reshape(block),
        parameters.reshape(whole),
        offsets.reshape(1, tensors + 1),
    )
    return new_parameters.reshape(parameters.shape), new_momentum.reshape(momentum.shape)


def solution(mesh):
    finer = Mesh(mesh.devices.reshape(2, 8, 2, 8, 2), AXES)
    sizes = dict(finer.shape)
    return jax.shard_map(
        functools.partial(on_device, sizes),
        mesh=finer,
        in_specs=(P(REP, SHARD), P(), P(SHARD), P(SHARD_REP)),
        out_specs=(P(SHARD), P(SHARD_REP)),
        check_vma=False,
    )
```

```python
import functools

import jax
import jax.numpy as jnp
from jax import lax
from jax.experimental import pallas as pl
from jax.experimental.pallas import tpu as pltpu
from jax.sharding import Mesh
from jax.sharding import PartitionSpec as P

X, Z, CORE, Y, XH = "rep_0", "rep_1", "rep_2", "shard_0", "shard_1"
AXES = (X, Z, CORE, Y, XH)
REP = (X, Z, CORE)
SHARD = (Y, XH)
SHARD_REP = (Y, XH, X, Z, CORE)

LR_OUTER = 0.7
MU_OUTER = 0.9
CLIP_RMS = 0.1
EPSILON = 1e-06


def remote(src, dst, send, recv, dev):
    return pltpu.make_async_remote_copy(
        src_ref=src,
        dst_ref=dst,
        send_sem=send,
        recv_sem=recv,
        device_id=dev,
        device_id_type=pl.DeviceIdType.MESH,
    )


def rs_order(half):
    order = [half]
    for d in range(half - 1, 0, -1):
        order += [-d, d]
    if half > 2:
        order.remove(half - 1)
        order.insert(half, half - 1)
    return order + [0]


def ag_order(half):
    return [e * d for d in range(1, half) for e in (1, -1)]


def step_kernel(
    sizes,
    delta, mom, par, offs,
    newp, newm,
    dl, sib, xs, xr, zs, zr, ar, ga, gm, pv, ov, hot, fac, sq1, sq2,
    lsem, c_send, c_far, c_near, x_send, x_recv, z_send, z_recv, a_send, a_recv,
    gz_send, gz_recv, gx_send, gx_recv, gc_send, gc_col, gc_recv,
    mx_send, mx_recv, mz_send, mz_recv, mc_send, mc_recv, q_send, q_recv,
):
    nx, nz, nc, ny, nh = (sizes[a] for a in AXES)
    x, z, c, y, h = (lax.axis_index(a) for a in AXES)
    rows = xs.shape[1]
    nq, half = nx * nz, nz // 2
    scope = jax.named_scope
    s = 1 - 2 * c
    zof = lambda d: lax.rem(z + s * d + nz, nz)
    mine, near, away = x * nz + z, x * nz, (1 - x) * nz
    x_nb, c_nb = {X: 1 - x}, {CORE: 1 - c}
    z_dev = lambda d: {Z: zof(d)}

    barrier = pltpu.get_barrier_semaphore()
    peers1 = [
        {Y: lax.rem(y + a, ny), CORE: lax.rem(c + b, nc)}
        for a in range(ny) for b in range(nc) if a or b
    ]
    peers2 = [
        {XH: lax.rem(h + a, nh), X: lax.rem(x + b, nx), Z: lax.rem(z + e, nz)}
        for a in range(nh) for b in range(nx) for e in range(nz) if a or b or e
    ]
    load_m = pltpu.make_async_copy(mom, gm.at[mine, c], lsem.at[0])
    load_m.start()
    load_away = pltpu.make_async_copy(delta.at[:, pl.ds(1 - c, 1)], dl.at[:, pl.ds(1 - c, 1)], lsem.at[1])
    load_away.start()
    load_own = pltpu.make_async_copy(delta.at[:, pl.ds(c, 1)], dl.at[:, pl.ds(c, 1)], lsem.at[2])
    load_own.start()
    with scope("signal"):
        for dev in peers1 + peers2:
            pl.semaphore_signal(barrier, inc=1, device_id=dev, device_id_type=pl.DeviceIdType.MESH)
    load_o = pltpu.make_async_copy(offs, ov, lsem.at[3])
    load_o.start()
    load_p = pltpu.make_async_copy(par, pv, lsem.at[4])
    load_p.start()
    with scope("load"):
        load_m.wait()
        load_away.wait()
    with scope("barrier"):
        pl.semaphore_wait(barrier, len(peers1) + len(peers2))

    def send(src, dst, send_sem, recv_sem, dev):
        remote(src, dst, send_sem, recv_sem, dev).start()

    def sent(ref, send_sem):
        remote(ref, ref, send_sem, send_sem, c_nb).wait_send()

    def came(ref, recv_sem):
        remote(ref, ref, recv_sem, recv_sem, c_nb).wait_recv()

    def all_of(ref, count):
        return ref.at[pl.ds(0, count)]

    send(gm.at[mine, c], gm.at[mine, c], mx_send, mx_recv, x_nb)

    def momentum_send(d, to, i):
        for first in (near, away):
            blk = gm.at[first + zof(d), c]
            send(blk, blk, mz_send, mz_recv.at[i], z_dev(to))

    def momentum_step(k):
        if k > 1:
            came(all_of(xs, 2), mz_recv.at[k - 2])
            if k <= half:
                came(all_of(xs, 2), mz_recv.at[half + k - 2])
        if k <= half:
            momentum_send(1 - k, 1, k - 1)
        if k < half:
            momentum_send(k - 1, -1, half + k - 1)

    steps = rs_order(half)
    with scope("core_send"):
        for i in range(nz):
            q = away + zof(-steps[i])
            send(dl.at[q, 1 - c], sib.at[q], c_send, c_far.at[i], c_nb)
        column = pl.ds(near, nz)
        send(dl.at[column, 1 - c], sib.at[column], c_send, c_near, c_nb)
        load_own.wait()

    with scope("x_stage"):
        for i in range(nz):
            q = away + zof(steps[i])
            came(sib.at[q], c_far.at[i])
            xs[i] = dl[q, c] + sib[q]
            send(xs.at[i], xr.at[i], x_send, x_recv.at[i], x_nb)

    own_len = rows * 128
    shard_pos = (y * nh + h) * (nq * nc * own_len)
    tensors = ov.shape[1] - 1
    with scope("one_hot"):
        load_o.wait()
        low, high = ov[:, 0:tensors], ov[:, 1 : tensors + 1]
        low, high = jnp.concatenate([low, low], axis=1), jnp.concatenate([high, high], axis=1)
        lanes = 2 * tensors

        def row_mask(first_pos):
            pos = first_pos + 128 * lax.broadcasted_iota(jnp.int32, (rows, lanes), 0)
            return (pos >= low) & (pos < high)

        for b in range(nq * nc):
            inside = row_mask(shard_pos + b * own_len)
            hot[pl.ds(b * rows, rows), :] = jnp.where(inside, 1.0, 0.0).astype(jnp.bfloat16)

    with scope("m1"):
        came(gm.at[away + z, c], mx_recv)
        momentum_step(1)

    came(sib.at[column], c_near)
    for i in range(nz):
        d = steps[i]
        with scope(f"z_stage{i}"):
            q = near + zof(d)
            came(xr.at[i], x_recv.at[i])
            part = dl[q, c] + sib[q] + xr[i]
            if d == half - 1:
                came(ar, a_recv)
                part = part + ar[...]
            zs[i] = part
            if i == 0:
                send(zs.at[i], ar, a_send, a_recv, z_dev(1))
            elif d != 0:
                send(zs.at[i], zr.at[i - 1], z_send, z_recv, z_dev(d))
        if i == half:
            with scope("m2"):
                momentum_step(2)
    with scope("m3"):
        if half > 2:
            momentum_step(3)

    with scope("z_sum"):
        came(zr, z_recv)
        total = zs[nz - 1]
        for i in range(nz - 2):
            total = total + zr[i]
        avg = total * (1.0 / (nq * nc))
        ga[mine, c] = avg

    slot1 = y * nc + c
    with scope("squares"):
        squares = jnp.sum(avg * avg, axis=1, keepdims=True)
        mask = row_mask(shard_pos + (mine * nc + c) * own_len)
        sq1[slot1] = jnp.sum(jnp.where(mask, squares, 0.0), axis=0, keepdims=True)
        for dev in peers1:
            send(sq1.at[slot1], sq1.at[slot1], q_send.at[0], q_recv.at[0], dev)

    hops = ag_order(half)
    nh_ = len(hops)
    own = ga.at[mine, c]
    with scope("ag_send"):
        for i, d in enumerate(hops):
            send(own, own, gz_send, gz_recv.at[i], z_dev(d))
        send(own, own, gx_send, gx_recv.at[nh_ + 1], x_nb)

    def mean_from_z(i):
        d = hops[i] if i < nh_ else half
        blk = ga.at[near + zof(-d), c]
        came(blk, gz_recv.at[i])
        if d == half - 1:
            send(blk, blk, gz_send, gz_recv.at[nh_], z_dev(1))
        send(blk, blk, gx_send, gx_recv.at[i], x_nb)

    def mean_from_x(i):
        d = 0 if i > nh_ else half if i == nh_ else hops[i]
        blk = ga.at[away + zof(-d), c]
        came(blk, gx_recv.at[i])
        send(blk, blk, gc_send, gc_recv.at[i], c_nb)

    for i in range(min(2, nh_)):
        with scope(f"ag_z{i}"):
            mean_from_z(i)

    slot2 = (h * nx + x) * nz + z
    with scope("q1"):
        came(all_of(sq1, ny * nc - 1), q_recv.at[0])
        acc = sq1[0]
        for i in range(1, ny * nc):
            acc = acc + sq1[i]
        sq2[slot2] = acc
        for dev in peers2:
            send(sq2.at[slot2], sq2.at[slot2], q_send.at[1], q_recv.at[1], dev)

    for i in range(2, nh_):
        with scope(f"ag_z{i}"):
            mean_from_z(i)
    with scope("ag_x_own"):
        mean_from_x(nh_ + 1)
    with scope("m4"):
        for k in range(4, half + 1):
            momentum_step(k)
    with scope("ag_z_far"):
        mean_from_z(nh_)
        send(ga.at[column, c], ga.at[column, c], gc_send, gc_col, c_nb)
    for i in range(2):
        with scope(f"ag_x{i}"):
            mean_from_x(i)
    with scope("m5"):
        momentum_step(half + 1)
        send(gm.at[:, c], gm.at[:, c], mc_send, mc_recv, c_nb)
    for i in range(2, nh_ + 1):
        with scope(f"ag_x{i}"):
            mean_from_x(i)

    with scope("q2"):
        came(all_of(sq2, nh * nq - 1), q_recv.at[1])
        acc = sq2[0]
        for i in range(1, nh * nq):
            acc = acc + sq2[i]
    with scope("factor"):
        lengths = (high - low).astype(jnp.float32)
        factor = jnp.minimum(1.0, CLIP_RMS * jnp.sqrt(lengths) * lax.rsqrt(acc + EPSILON))
        at = lambda axis: lax.broadcasted_iota(jnp.int32, (tensors, lanes), axis)
        spread = jnp.sum(jnp.where(at(0) == at(1), factor, 0.0), axis=1, keepdims=True)
        spread = jnp.broadcast_to(spread, (tensors, 128))
        upper = spread.astype(jnp.bfloat16)
        fac[0:tensors, :] = upper
        fac[tensors:lanes, :] = (spread - upper.astype(jnp.float32)).astype(jnp.bfloat16)
        table = fac[...]

    with scope("m_core"):
        came(gm.at[:, 1 - c], mc_recv)
    with scope("base"):
        load_p.wait()
        for q in range(nq):
            pv[q] = pv[q] - (LR_OUTER * MU_OUTER * MU_OUTER) * gm[q]

    with scope("ag_core"):
        came(ga.at[column, 1 - c], gc_col)
        for i in range(nz):
            d = 0 if i > nh_ else half if i == nh_ else hops[i]
            came(ga.at[away + zof(d), 1 - c], gc_recv.at[i])

    with scope("apply"):
        step = 2
        for b in range(0, nq, step):
            spread = jnp.dot(
                hot[pl.ds(b * nc * rows, step * nc * rows), :], table, preferred_element_type=jnp.float32
            ).reshape(step, nc, rows, 128)
            part = pl.ds(b, step)
            newp[part] = pv[part] - (LR_OUTER * (1.0 + MU_OUTER)) * (ga[part] * spread)
        first = pl.multiple_of((mine * nc + c) * rows, rows)
        spread = jnp.dot(hot[pl.ds(first, rows), :], table, preferred_element_type=jnp.float32)
        newm[...] = MU_OUTER * gm[mine, c] + ga[mine, c] * spread

    with scope("drain"):
        sent(sib, c_send)
        sent(xs, x_send)
        sent(zr, z_send)
        sent(ar, a_send)
        sent(all_of(xs, nz - 1), gz_send)
        sent(xs, gx_send)
        sent(sib, gc_send)
        sent(ar, mx_send)
        sent(all_of(sib, 2 * (nz - 1)), mz_send)
        sent(sib, mc_send)
        sent(all_of(sq1, ny * nc - 1), q_send.at[0])
        sent(all_of(sq2, nh * nq - 1), q_send.at[1])


def write_out(newp, newm, out_p, out_m, sem):
    copies = [pltpu.make_async_copy(newp, out_p, sem.at[0]), pltpu.make_async_copy(newm, out_m, sem.at[1])]
    for copy in copies:
        copy.start()
    for copy in copies:
        copy.wait()


VMEM_LIMIT = 52 * 1024 * 1024


def on_device(sizes, outer_delta, offsets, parameters, momentum):
    nx, nz, nc, ny, nh = (sizes[a] for a in AXES)
    rows = momentum.shape[0] // 128
    nq = nx * nz
    whole = (nq, nc, rows, 128)
    block = (rows, 128)
    f32 = jnp.float32
    dma = lambda *n: pltpu.SemaphoreType.DMA(n)
    vmem = pltpu.VMEM
    tensors = offsets.shape[0] - 1
    outs = (jax.ShapeDtypeStruct(whole, f32), jax.ShapeDtypeStruct(block, f32))
    in_vmem = (pl.BlockSpec(memory_space=pltpu.VMEM),) * 2
    results = pl.pallas_call(
        functools.partial(step_kernel, sizes),
        out_shape=outs,
        in_specs=[pl.BlockSpec(memory_space=pltpu.HBM)] * 4,
        out_specs=in_vmem,
        scratch_shapes=[
            vmem(whole, f32),
            vmem((nq,) + block, f32),
            vmem((nz,) + block, f32),
            vmem((nz,) + block, f32),
            vmem((nz,) + block, f32),
            vmem((nz - 2,) + block, f32),
            vmem(block, f32),
            vmem(whole, f32),
            vmem(whole, f32),
            vmem(whole, f32),
            vmem((1, tensors + 1), jnp.int32),
            vmem((nq * nc * rows, 2 * tensors), jnp.bfloat16),
            vmem((2 * tensors, 128), jnp.bfloat16),
            vmem((ny * nc, 1, 2 * tensors), f32),
            vmem((nh * nq, 1, 2 * tensors), f32),
            dma(5),
            dma(), dma(nz), dma(),
            dma(), dma(nz),
            dma(), dma(), dma(), dma(),
            dma(), dma(nz - 1), dma(), dma(nz), dma(), dma(), dma(nz),
            dma(), dma(), dma(), dma(nz - 1), dma(), dma(),
            dma(2), dma(2),
        ],
        compiler_params=pltpu.CompilerParams(
            collective_id=0, has_side_effects=True, vmem_limit_bytes=VMEM_LIMIT
        ),
    )(
        outer_delta.reshape(whole),
        momentum.reshape(block),
        parameters.reshape(whole),
        offsets.reshape(1, tensors + 1),
    )
    new_parameters, new_momentum = pl.pallas_call(
        write_out,
        out_shape=outs,
        in_specs=list(in_vmem),
        out_specs=(pl.BlockSpec(memory_space=pl.ANY),) * 2,
        scratch_shapes=[dma(2)],
        compiler_params=pltpu.CompilerParams(vmem_limit_bytes=4 * 1024 * 1024),
    )(*results)
    return new_parameters.reshape(parameters.shape), new_momentum.reshape(momentum.shape)


def solution(mesh):
    finer = Mesh(mesh.devices.reshape(2, 8, 2, 8, 2), AXES)
    sizes = dict(finer.shape)
    return jax.shard_map(
        functools.partial(on_device, sizes),
        mesh=finer,
        in_specs=(P(REP, SHARD), P(), P(SHARD), P(SHARD_REP)),
        out_specs=(P(SHARD), P(SHARD_REP)),
        check_vma=False,
    )
```

```python
import functools

import jax
import jax.numpy as jnp
from jax import lax
from jax.experimental import pallas as pl
from jax.experimental.pallas import tpu as pltpu
from jax.sharding import Mesh
from jax.sharding import PartitionSpec as P

X, Z, CORE, Y, XH = "rep_0", "rep_1", "rep_2", "shard_0", "shard_1"
AXES = (X, Z, CORE, Y, XH)
REP = (X, Z, CORE)
SHARD = (Y, XH)
SHARD_REP = (Y, XH, X, Z, CORE)

LR_OUTER = 0.7
MU_OUTER = 0.9
CLIP_RMS = 0.1
EPSILON = 1e-06


def remote(src, dst, send, recv, dev):
    return pltpu.make_async_remote_copy(
        src_ref=src,
        dst_ref=dst,
        send_sem=send,
        recv_sem=recv,
        device_id=dev,
        device_id_type=pl.DeviceIdType.MESH,
    )


def rs_order(half):
    order = [half]
    for d in range(half - 1, 0, -1):
        order += [-d, d]
    if half > 2:
        order.remove(half - 1)
        order.insert(half, half - 1)
    return order + [0]


def step_kernel(
    sizes,
    delta, mom, par, offs,
    newp, newm,
    dl, sib, xs, xr, zs, zr, ar, ga, gm, pv, ov, hot, fac, sq1, sq2,
    lsem, c_send, c_far, c_near, x_send, x_recv, z_send, z_recv, a_send, a_recv,
    gz_send, gz_recv, gx_send, gx_recv, gc_send, gc_col, gc_recv,
    mx_send, mx_recv, mz_send, mz_recv, mc_send, mc_recv, q_send, q_recv, in_column, in_peers,
):
    nx, nz, nc, ny, nh = (sizes[a] for a in AXES)
    x, z, c, y, h = (lax.axis_index(a) for a in AXES)
    rows = xs.shape[1]
    nq, half = nx * nz, nz // 2
    scope = jax.named_scope
    s = 1 - 2 * c
    zof = lambda d: lax.rem(z + s * d + nz, nz)
    mine, near, away = x * nz + z, x * nz, (1 - x) * nz
    column = pl.ds(near, nz)
    x_nb, c_nb = {X: 1 - x}, {CORE: 1 - c}
    z_dev = lambda d: {Z: zof(d)}

    barrier = pltpu.get_barrier_semaphore()
    peers1 = [
        {Y: lax.rem(y + a, ny), CORE: lax.rem(c + b, nc)}
        for a in range(ny) for b in range(nc) if a or b
    ]
    peers2 = [
        {XH: lax.rem(h + a, nh), X: lax.rem(x + b, nx), Z: lax.rem(z + e, nz)}
        for a in range(nh) for b in range(nx) for e in range(nz) if a or b or e
    ]
    row = [
        {XH: lax.rem(h + a, nh), X: lax.rem(x + b, nx)}
        for a in range(nh) for b in range(nx) if a or b
    ]
    cores = [{CORE: e} for e in range(nc)]

    def tell(sem, dev):
        pl.semaphore_signal(sem, inc=1, device_id=dev, device_id_type=pl.DeviceIdType.MESH)

    def tell_each(sem, axis, first, last, devs):
        def at(i, carry):
            for dev in devs:
                tell(sem, dev | {axis: i})
            return carry

        lax.fori_loop(first, last, at, 0)

    def wait_for(sem, count):
        @pl.when(count > 0)
        def _():
            pl.semaphore_wait(sem, count)

    load_m = pltpu.make_async_copy(mom, gm.at[mine, c], lsem.at[0])
    load_m.start()
    load_away = pltpu.make_async_copy(delta.at[:, pl.ds(1 - c, 1)], dl.at[:, pl.ds(1 - c, 1)], lsem.at[1])
    load_away.start()
    load_own = pltpu.make_async_copy(delta.at[:, pl.ds(c, 1)], dl.at[:, pl.ds(c, 1)], lsem.at[2])
    load_own.start()
    with scope("signal"):
        for dev in [c_nb] + row:
            tell(barrier, dev)
        tell_each(barrier, Z, z + 1, nz, [{}] + row)
        tell_each(barrier, Y, y + 1, ny, cores)
    load_o = pltpu.make_async_copy(offs, ov, lsem.at[3])
    load_o.start()
    load_p = pltpu.make_async_copy(par, pv, lsem.at[4])
    load_p.start()
    with scope("load"):
        load_m.wait()
        load_away.wait()
    with scope("barrier"):
        pl.semaphore_wait(barrier, 1 + len(row) + y * nc + z * (1 + len(row)))
        tell_each(in_column, Z, 0, z, [{}])

    def send(src, dst, send_sem, recv_sem, dev):
        remote(src, dst, send_sem, recv_sem, dev).start()

    def sent(ref, send_sem):
        remote(ref, ref, send_sem, send_sem, c_nb).wait_send()

    def came(ref, recv_sem):
        remote(ref, ref, recv_sem, recv_sem, c_nb).wait_recv()

    def all_of(ref, count):
        return ref.at[pl.ds(0, count)]

    own_m = gm.at[mine, c]
    near_m = [e * d for d in range(1, max(half - 1, 2)) for e in (1, -1)]
    last = near_m[-2]
    passed = [(-last, 1), (-last, 2), (last, -1)] if half > 2 else [(-last, 1)]
    send(own_m, own_m, mx_send, mx_recv, x_nb)
    def momentum_across(d):
        blk = gm.at[near + zof(d), c]
        send(blk, blk, mx_send, mx_recv, x_nb)

    def momentum_near():
        came(all_of(xs, len(near_m)), mz_recv.at[0])
        for d, to in passed:
            blk = gm.at[near + zof(d), c]
            send(blk, blk, mz_send, mz_recv.at[1], z_dev(to))
        for d in near_m:
            momentum_across(-d)

    def momentum_far():
        came(all_of(xs, len(passed)), mz_recv.at[1])
        for d, to in passed:
            momentum_across(d - to)
        send(gm.at[column, c], gm.at[column, c], mc_send, mc_recv, c_nb)

    steps = rs_order(half)
    with scope("core_send"):
        for i in range(nz):
            q = away + zof(-steps[i])
            send(dl.at[q, 1 - c], sib.at[q], c_send, c_far.at[i], c_nb)
        send(dl.at[column, 1 - c], sib.at[column], c_send, c_near, c_nb)
        load_own.wait()

    with scope("tell"):
        tell_each(in_peers, Z, 0, z, row)
        tell_each(in_peers, Y, 0, y, cores)
    with scope("x_stage"):
        for i in range(nz):
            q = away + zof(steps[i])
            came(sib.at[q], c_far.at[i])
            xs[i] = dl[q, c] + sib[q]
            send(xs.at[i], xr.at[i], x_send, x_recv.at[i], x_nb)

    own_len = rows * 128
    shard_pos = (y * nh + h) * (nq * nc * own_len)
    tensors = ov.shape[1] - 1
    with scope("one_hot"):
        load_o.wait()
        low, high = ov[:, 0:tensors], ov[:, 1 : tensors + 1]
        low, high = jnp.concatenate([low, low], axis=1), jnp.concatenate([high, high], axis=1)
        lanes = 2 * tensors

        def row_mask(first_pos):
            pos = first_pos + 128 * lax.broadcasted_iota(jnp.int32, (rows, lanes), 0)
            return (pos >= low) & (pos < high)

        for b in range(nq * nc):
            inside = row_mask(shard_pos + b * own_len)
            hot[pl.ds(b * rows, rows), :] = jnp.where(inside, 1.0, 0.0).astype(jnp.bfloat16)

    with scope("column"):
        wait_for(in_column, nz - 1 - z)
        for d in near_m:
            send(own_m, own_m, mz_send, mz_recv.at[0], z_dev(d))
    came(sib.at[column], c_near)
    for i in range(nz):
        d = steps[i]
        with scope(f"z_stage{i}"):
            q = near + zof(d)
            came(xr.at[i], x_recv.at[i])
            part = dl[q, c] + sib[q] + xr[i]
            if d == half - 1:
                came(ar, a_recv)
                part = part + ar[...]
            zs[i] = part
            if i == 0:
                send(zs.at[i], ar, a_send, a_recv, z_dev(1))
            elif d != 0:
                send(zs.at[i], zr.at[i - 1], z_send, z_recv, z_dev(d))
    with scope("m_near"):
        momentum_near()

    with scope("z_sum"):
        came(zr, z_recv)
        total = zs[nz - 1]
        for i in range(nz - 2):
            total = total + zr[i]
        avg = total * (1.0 / (nq * nc))
        ga[mine, c] = avg

    slot1 = y * nc + c
    with scope("squares"):
        squares = jnp.sum(avg * avg, axis=1, keepdims=True)
        mask = row_mask(shard_pos + (mine * nc + c) * own_len)
        sq1[slot1] = jnp.sum(jnp.where(mask, squares, 0.0), axis=0, keepdims=True)
        wait_for(in_peers, (ny - 1 - y) * nc + (nz - 1 - z) * len(row))
        for dev in peers1:
            send(sq1.at[slot1], sq1.at[slot1], q_send.at[0], q_recv.at[0], dev)

    own = ga.at[mine, c]
    from_z = [-d for d in near_m] + [d - to for d, to in passed]
    origins = from_z + [0]
    with scope("ag_send"):
        for i, d in enumerate(near_m):
            send(own, own, gz_send, gz_recv.at[i], z_dev(d))
        send(own, own, gx_send, gx_recv.at[nz - 1], x_nb)

    def mean_from_z(i):
        blk = ga.at[near + zof(from_z[i]), c]
        came(blk, gz_recv.at[i])
        for k, (d, to) in enumerate(passed):
            if d == from_z[i]:
                send(blk, blk, gz_send, gz_recv.at[len(near_m) + k], z_dev(to))
        send(blk, blk, gx_send, gx_recv.at[i], x_nb)

    def mean_from_x(i):
        blk = ga.at[away + zof(origins[i]), c]
        came(blk, gx_recv.at[i])
        send(blk, blk, gc_send, gc_recv.at[i], c_nb)

    with scope("m_far"):
        momentum_far()
    for i in range(len(near_m)):
        with scope(f"ag_z{i}"):
            mean_from_z(i)

    slot2 = (h * nx + x) * nz + z
    with scope("q1"):
        came(all_of(sq1, ny * nc - 1), q_recv.at[0])
        acc = sq1[0]
        for i in range(1, ny * nc):
            acc = acc + sq1[i]
        sq2[slot2] = acc
        for dev in peers2:
            send(sq2.at[slot2], sq2.at[slot2], q_send.at[1], q_recv.at[1], dev)

    with scope("ag_x_own"):
        mean_from_x(nz - 1)
    for i in range(2):
        with scope(f"ag_x{i}"):
            mean_from_x(i)
    for i in range(len(near_m), nz - 1):
        with scope(f"ag_z{i}"):
            mean_from_z(i)
    send(ga.at[column, c], ga.at[column, c], gc_send, gc_col, c_nb)
    with scope("m_x"):
        other = gm.at[pl.ds(away, nz), c]
        came(other, mx_recv)
        send(other, other, mc_send, mc_recv, c_nb)
    for i in range(2, nz - 1):
        with scope(f"ag_x{i}"):
            mean_from_x(i)

    with scope("q2"):
        came(all_of(sq2, nh * nq - 1), q_recv.at[1])
        acc = sq2[0]
        for i in range(1, nh * nq):
            acc = acc + sq2[i]
    with scope("factor"):
        lengths = (high - low).astype(jnp.float32)
        factor = jnp.minimum(1.0, CLIP_RMS * jnp.sqrt(lengths) * lax.rsqrt(acc + EPSILON))
        at = lambda axis: lax.broadcasted_iota(jnp.int32, (tensors, lanes), axis)
        spread = jnp.sum(jnp.where(at(0) == at(1), factor, 0.0), axis=1, keepdims=True)
        spread = jnp.broadcast_to(spread, (tensors, 128))
        upper = spread.astype(jnp.bfloat16)
        fac[0:tensors, :] = upper
        fac[tensors:lanes, :] = (spread - upper.astype(jnp.float32)).astype(jnp.bfloat16)
        table = fac[...]

    with scope("m_core"):
        came(gm.at[:, 1 - c], mc_recv)
    with scope("base"):
        load_p.wait()
        for q in range(nq):
            pv[q] = pv[q] - (LR_OUTER * MU_OUTER * MU_OUTER) * gm[q]

    with scope("ag_core"):
        came(ga.at[column, 1 - c], gc_col)
        for i in range(nz):
            came(ga.at[away + zof(-origins[i]), 1 - c], gc_recv.at[i])

    with scope("apply"):
        step = 2
        for b in range(0, nq, step):
            spread = jnp.dot(
                hot[pl.ds(b * nc * rows, step * nc * rows), :], table, preferred_element_type=jnp.float32
            ).reshape(step, nc, rows, 128)
            part = pl.ds(b, step)
            newp[part] = pv[part] - (LR_OUTER * (1.0 + MU_OUTER)) * (ga[part] * spread)
        first = pl.multiple_of((mine * nc + c) * rows, rows)
        spread = jnp.dot(hot[pl.ds(first, rows), :], table, preferred_element_type=jnp.float32)
        newm[...] = MU_OUTER * gm[mine, c] + ga[mine, c] * spread

    with scope("drain"):
        sent(sib, c_send)
        sent(xs, x_send)
        sent(zr, z_send)
        sent(ar, a_send)
        sent(all_of(xs, nz - 1), gz_send)
        sent(xs, gx_send)
        sent(sib, gc_send)
        sent(xs, mx_send)
        sent(all_of(xs, nz - 1), mz_send)
        sent(sib, mc_send)
        sent(all_of(sq1, ny * nc - 1), q_send.at[0])
        sent(all_of(sq2, nh * nq - 1), q_send.at[1])


def write_out(newp, newm, out_p, out_m, sem):
    copies = [pltpu.make_async_copy(newp, out_p, sem.at[0]), pltpu.make_async_copy(newm, out_m, sem.at[1])]
    for copy in copies:
        copy.start()
    for copy in copies:
        copy.wait()


VMEM_LIMIT = 52 * 1024 * 1024


def on_device(sizes, outer_delta, offsets, parameters, momentum):
    nx, nz, nc, ny, nh = (sizes[a] for a in AXES)
    rows = momentum.shape[0] // 128
    nq = nx * nz
    whole = (nq, nc, rows, 128)
    block = (rows, 128)
    f32 = jnp.float32
    dma = lambda *n: pltpu.SemaphoreType.DMA(n)
    vmem = pltpu.VMEM
    tensors = offsets.shape[0] - 1
    outs = (jax.ShapeDtypeStruct(whole, f32), jax.ShapeDtypeStruct(block, f32))
    in_vmem = (pl.BlockSpec(memory_space=pltpu.VMEM),) * 2
    results = pl.pallas_call(
        functools.partial(step_kernel, sizes),
        out_shape=outs,
        in_specs=[pl.BlockSpec(memory_space=pltpu.HBM)] * 4,
        out_specs=in_vmem,
        scratch_shapes=[
            vmem(whole, f32),
            vmem((nq,) + block, f32),
            vmem((nz,) + block, f32),
            vmem((nz,) + block, f32),
            vmem((nz,) + block, f32),
            vmem((nz - 2,) + block, f32),
            vmem(block, f32),
            vmem(whole, f32),
            vmem(whole, f32),
            vmem(whole, f32),
            vmem((1, tensors + 1), jnp.int32),
            vmem((nq * nc * rows, 2 * tensors), jnp.bfloat16),
            vmem((2 * tensors, 128), jnp.bfloat16),
            vmem((ny * nc, 1, 2 * tensors), f32),
            vmem((nh * nq, 1, 2 * tensors), f32),
            dma(5),
            dma(), dma(nz), dma(),
            dma(), dma(nz),
            dma(), dma(), dma(), dma(),
            dma(), dma(nz - 1), dma(), dma(nz), dma(), dma(), dma(nz),
            dma(), dma(), dma(), dma(2), dma(), dma(),
            dma(2), dma(2), pltpu.SemaphoreType.REGULAR, pltpu.SemaphoreType.REGULAR,
        ],
        compiler_params=pltpu.CompilerParams(
            collective_id=0, has_side_effects=True, vmem_limit_bytes=VMEM_LIMIT
        ),
    )(
        outer_delta.reshape(whole),
        momentum.reshape(block),
        parameters.reshape(whole),
        offsets.reshape(1, tensors + 1),
    )
    new_parameters, new_momentum = pl.pallas_call(
        write_out,
        out_shape=outs,
        in_specs=list(in_vmem),
        out_specs=(pl.BlockSpec(memory_space=pl.ANY),) * 2,
        scratch_shapes=[dma(2)],
        compiler_params=pltpu.CompilerParams(vmem_limit_bytes=4 * 1024 * 1024),
    )(*results)
    return new_parameters.reshape(parameters.shape), new_momentum.reshape(momentum.shape)


def solution(mesh):
    finer = Mesh(mesh.devices.reshape(2, 8, 2, 8, 2), AXES)
    sizes = dict(finer.shape)
    return jax.shard_map(
        functools.partial(on_device, sizes),
        mesh=finer,
        in_specs=(P(REP, SHARD), P(), P(SHARD), P(SHARD_REP)),
        out_specs=(P(SHARD), P(SHARD_REP)),
        check_vma=False,
    )
```

```python
import functools

import jax
import jax.numpy as jnp
from jax import lax
from jax.experimental import pallas as pl
from jax.experimental.pallas import tpu as pltpu
from jax.sharding import Mesh
from jax.sharding import PartitionSpec as P

X, Z, CORE, Y, XH = "rep_0", "rep_1", "rep_2", "shard_0", "shard_1"
AXES = (X, Z, CORE, Y, XH)
REP = (X, Z, CORE)
SHARD = (Y, XH)
SHARD_REP = (Y, XH, X, Z, CORE)

LR_OUTER = 0.7
MU_OUTER = 0.9
CLIP_RMS = 0.1
EPSILON = 1e-06


def remote(src, dst, send, recv, dev):
    return pltpu.make_async_remote_copy(
        src_ref=src,
        dst_ref=dst,
        send_sem=send,
        recv_sem=recv,
        device_id=dev,
        device_id_type=pl.DeviceIdType.MESH,
    )


def rs_order(half):
    order = [half]
    for d in range(half - 1, 0, -1):
        order += [-d, d]
    if half > 2:
        order.remove(half - 1)
        order.insert(half, half - 1)
    return order + [0]


def step_kernel(
    sizes,
    delta, mom, par, offs,
    newp, newm,
    dl, sib, xs, xr, zs, zr, ar, ga, gm, pv, ov, hot, fac, sq1, sq2,
    lsem, c_send, c_far, c_near, x_send, x_recv, z_send, z_recv, a_send, a_recv,
    gz_send, gz_recv, gx_send, gx_recv, gc_send, gc_col, gc_recv,
    mx_send, mx_recv, mz_send, mz_recv, mc_send, mc_recv, q_send, q_recv, in_column, in_peers,
):
    nx, nz, nc, ny, nh = (sizes[a] for a in AXES)
    x, z, c, y, h = (lax.axis_index(a) for a in AXES)
    rows = xs.shape[1]
    nq, half = nx * nz, nz // 2
    scope = jax.named_scope
    s = 1 - 2 * c
    zof = lambda d: lax.rem(z + s * d + nz, nz)
    mine, near, away = x * nz + z, x * nz, (1 - x) * nz
    column = pl.ds(near, nz)
    x_nb, c_nb = {X: 1 - x}, {CORE: 1 - c}
    z_dev = lambda d: {Z: zof(d)}

    barrier = pltpu.get_barrier_semaphore()
    peers1 = [
        {Y: lax.rem(y + a, ny), CORE: lax.rem(c + b, nc)}
        for a in range(ny) for b in range(nc) if a or b
    ]
    peers2 = [
        {XH: lax.rem(h + a, nh), X: lax.rem(x + b, nx), Z: lax.rem(z + e, nz)}
        for a in range(nh) for b in range(nx) for e in range(nz) if a or b or e
    ]
    row = [
        {XH: lax.rem(h + a, nh), X: lax.rem(x + b, nx)}
        for a in range(nh) for b in range(nx) if a or b
    ]
    pair = [{X: b} for b in range(nx)]
    cores = [{CORE: e} for e in range(nc)]

    def tell(sem, dev):
        pl.semaphore_signal(sem, inc=1, device_id=dev, device_id_type=pl.DeviceIdType.MESH)

    def tell_each(sem, axis, first, last, devs):
        def at(i, carry):
            for dev in devs:
                tell(sem, dev | {axis: i})
            return carry

        lax.fori_loop(first, last, at, 0)

    def wait_for(sem, count):
        @pl.when(count > 0)
        def _():
            pl.semaphore_wait(sem, count)

    load_m = pltpu.make_async_copy(mom, gm.at[mine, c], lsem.at[0])
    load_m.start()
    load_away = pltpu.make_async_copy(delta.at[:, pl.ds(1 - c, 1)], dl.at[:, pl.ds(1 - c, 1)], lsem.at[1])
    load_away.start()
    load_own = pltpu.make_async_copy(delta.at[:, pl.ds(c, 1)], dl.at[:, pl.ds(c, 1)], lsem.at[2])
    load_own.start()
    with scope("signal"):
        for dev in (c_nb, x_nb):
            tell(barrier, dev)
        tell_each(barrier, XH, h + 1, nh, pair)
        tell_each(barrier, Z, z + 1, nz, [{}] + row)
        tell_each(barrier, Y, y + 1, ny, cores)
    load_o = pltpu.make_async_copy(offs, ov, lsem.at[3])
    load_o.start()
    load_p = pltpu.make_async_copy(par, pv, lsem.at[4])
    load_p.start()
    with scope("load"):
        load_m.wait()
        load_away.wait()
    with scope("barrier"):
        pl.semaphore_wait(barrier, 2 + h * nx + y * nc + z * (1 + len(row)))

        def tell_column(i, carry):
            tell(in_column.at[z - 1 - i], {Z: i})
            return carry

        lax.fori_loop(0, z, tell_column, 0)

    def send(src, dst, send_sem, recv_sem, dev):
        remote(src, dst, send_sem, recv_sem, dev).start()

    def sent(ref, send_sem):
        remote(ref, ref, send_sem, send_sem, c_nb).wait_send()

    def came(ref, recv_sem):
        remote(ref, ref, recv_sem, recv_sem, c_nb).wait_recv()

    def all_of(ref, count):
        return ref.at[pl.ds(0, count)]

    own_m = gm.at[mine, c]
    near_m = [e * d for d in range(1, max(half - 1, 2)) for e in (1, -1)]
    last = near_m[-2]
    passed = [(-last, 1), (-last, 2), (last, -1)] if half > 2 else [(-last, 1)]
    send(own_m, own_m, mx_send, mx_recv, x_nb)
    reach = max(near_m)

    def momentum_to(i, condition):
        @pl.when(condition)
        def _():
            send(own_m, own_m, mz_send, mz_recv.at[0], {Z: i})

    def momentum_across(d):
        blk = gm.at[near + zof(d), c]
        send(blk, blk, mx_send, mx_recv, x_nb)

    def momentum_near():
        came(all_of(xs, len(near_m)), mz_recv.at[0])
        for d, to in passed:
            blk = gm.at[near + zof(d), c]
            send(blk, blk, mz_send, mz_recv.at[1], z_dev(to))
        for d in near_m:
            momentum_across(-d)

    def momentum_far():
        came(all_of(xs, len(passed)), mz_recv.at[1])
        for d, to in passed:
            momentum_across(d - to)
        send(gm.at[column, c], gm.at[column, c], mc_send, mc_recv, c_nb)

    steps = rs_order(half)
    with scope("core_send"):
        for i in range(nz):
            q = away + zof(-steps[i])
            send(dl.at[q, 1 - c], sib.at[q], c_send, c_far.at[i], c_nb)
        send(dl.at[column, 1 - c], sib.at[column], c_send, c_near, c_nb)
        load_own.wait()

    with scope("m_smaller"):
        for d in near_m:
            momentum_to(zof(d), zof(d) < z)
    with scope("tell"):
        tell_each(in_peers, XH, 0, h, pair)
        tell_each(in_peers, Z, 0, z, row)
        tell_each(in_peers, Y, 0, y, cores)
    with scope("x_stage"):
        for i in range(nz):
            q = away + zof(steps[i])
            came(sib.at[q], c_far.at[i])
            xs[i] = dl[q, c] + sib[q]
            send(xs.at[i], xr.at[i], x_send, x_recv.at[i], x_nb)

    own_len = rows * 128
    shard_pos = (y * nh + h) * (nq * nc * own_len)
    tensors = ov.shape[1] - 1
    with scope("one_hot"):
        load_o.wait()
        low, high = ov[:, 0:tensors], ov[:, 1 : tensors + 1]
        low, high = jnp.concatenate([low, low], axis=1), jnp.concatenate([high, high], axis=1)
        lanes = 2 * tensors

        def row_mask(first_pos):
            pos = first_pos + 128 * lax.broadcasted_iota(jnp.int32, (rows, lanes), 0)
            return (pos >= low) & (pos < high)

        for b in range(nq * nc):
            inside = row_mask(shard_pos + b * own_len)
            hot[pl.ds(b * rows, rows), :] = jnp.where(inside, 1.0, 0.0).astype(jnp.bfloat16)

    with scope("column"):
        for e in range(1, nz):
            @pl.when(z + e < nz)
            def _(e=e):
                pl.semaphore_wait(in_column.at[e - 1], 1)

            if e <= reach:
                momentum_to(z + e, z + e < nz)
        for e in range(1, reach + 1):
            momentum_to(z - e + nz, z - e < 0)
    came(sib.at[column], c_near)
    for i in range(nz):
        d = steps[i]
        with scope(f"z_stage{i}"):
            q = near + zof(d)
            came(xr.at[i], x_recv.at[i])
            part = dl[q, c] + sib[q] + xr[i]
            if d == half - 1:
                came(ar, a_recv)
                part = part + ar[...]
            zs[i] = part
            if i == 0:
                send(zs.at[i], ar, a_send, a_recv, z_dev(1))
            elif d != 0:
                send(zs.at[i], zr.at[i - 1], z_send, z_recv, z_dev(d))
    with scope("m_near"):
        momentum_near()

    with scope("z_sum"):
        came(zr, z_recv)
        total = zs[nz - 1]
        for i in range(nz - 2):
            total = total + zr[i]
        avg = total * (1.0 / (nq * nc))
        ga[mine, c] = avg

    slot1 = y * nc + c
    with scope("squares"):
        squares = jnp.sum(avg * avg, axis=1, keepdims=True)
        mask = row_mask(shard_pos + (mine * nc + c) * own_len)
        sq1[slot1] = jnp.sum(jnp.where(mask, squares, 0.0), axis=0, keepdims=True)
        wait_for(in_peers, (nh - 1 - h) * nx + (ny - 1 - y) * nc + (nz - 1 - z) * len(row))
        for dev in peers1:
            send(sq1.at[slot1], sq1.at[slot1], q_send.at[0], q_recv.at[0], dev)

    own = ga.at[mine, c]
    hops = [e * d for d in list(range(2, half)) + [1] for e in (1, -1)]
    relay = -min(2, half - 1)
    from_z = [-d for d in hops] + [-half]
    origins = from_z + [0]
    beyond = [i for i in range(2, nz - 2) if abs(from_z[i]) > 1]
    beside = [i for i in range(2, nz - 2) if abs(from_z[i]) == 1]
    with scope("ag_send"):
        for i, d in enumerate(hops):
            if i in beside:
                continue
            send(own, own, gz_send, gz_recv.at[i], z_dev(d))
        send(own, own, gx_send, gx_recv.at[nz - 1], x_nb)

    def mean_from_z(i):
        blk = ga.at[near + zof(from_z[i]), c]
        came(blk, gz_recv.at[i])
        if from_z[i] == relay:
            send(blk, blk, gz_send, gz_recv.at[nz - 2], z_dev(half + relay))
        if abs(from_z[i]) > 1:
            send(blk, blk, gx_send, gx_recv.at[i], x_nb)

    def mean_beside():
        across = ga.at[away + z, c]
        for k, d in enumerate(from_z):
            if abs(d) == 1:
                if k in beside:
                    send(own, own, gz_send, gz_recv.at[k], z_dev(-d))
                send(across, across, gx_send, gx_recv.at[k], z_dev(-d))

    def mean_from_x(i):
        blk = ga.at[away + zof(origins[i]), c]
        came(blk, gx_recv.at[i])
        if origins[i] == 0 and half == 2:
            mean_beside()
        send(blk, blk, gc_send, gc_recv, c_nb)

    slot2 = (h * nx + x) * nz + z

    def exchange_squares(condition):
        @pl.when(condition)
        def _():
            with scope("q1"):
                came(all_of(sq1, ny * nc - 1), q_recv.at[0])
                acc = sq1[0]
                for i in range(1, ny * nc):
                    acc = acc + sq1[i]
                sq2[slot2] = acc
                for dev in peers2:
                    send(sq2.at[slot2], sq2.at[slot2], q_send.at[1], q_recv.at[1], dev)
                if half > 2:
                    mean_beside()

    with scope("m_far"):
        momentum_far()
    with scope("ag_x_own"):
        mean_from_x(nz - 1)
    exchange_squares(2 * y >= ny)
    for i in [0, 1] + beyond:
        with scope(f"ag_z{i}"):
            mean_from_z(i)

    exchange_squares(2 * y < ny)
    for i in [nz - 2] + beside:
        with scope(f"ag_z{i}"):
            mean_from_z(i)
    send(ga.at[column, c], ga.at[column, c], gc_send, gc_col, c_nb)
    with scope("drain1"):
        sent(sib, c_send)
        sent(xs, x_send)
        sent(zr, z_send)
        sent(ar, a_send)
        sent(all_of(xs, nz - 1), gz_send)
        sent(all_of(xs, nz - 1), mz_send)
        sent(all_of(sq1, ny * nc - 1), q_send.at[0])
    for i in [0, 1] + beside:
        with scope(f"ag_x{i}"):
            mean_from_x(i)
    with scope("m_x"):
        other = gm.at[pl.ds(away, nz), c]
        came(other, mx_recv)
        send(other, other, mc_send, mc_recv, c_nb)
    for i in beyond:
        with scope(f"ag_x{i}"):
            mean_from_x(i)

    with scope("m_core"):
        came(gm.at[:, 1 - c], mc_recv)
    with scope("base"):
        load_p.wait()
        for q in range(nq):
            pv[q] = pv[q] - (LR_OUTER * MU_OUTER * MU_OUTER) * gm[q]
    with scope("ag_x_far"):
        mean_from_x(nz - 2)

    with scope("q2"):
        came(all_of(sq2, nh * nq - 1), q_recv.at[1])
        acc = sq2[0]
        for i in range(1, nh * nq):
            acc = acc + sq2[i]
    with scope("factor"):
        lengths = (high - low).astype(jnp.float32)
        factor = jnp.minimum(1.0, CLIP_RMS * jnp.sqrt(lengths) * lax.rsqrt(acc + EPSILON))
        at = lambda axis: lax.broadcasted_iota(jnp.int32, (tensors, lanes), axis)
        spread = jnp.sum(jnp.where(at(0) == at(1), factor, 0.0), axis=1, keepdims=True)
        spread = jnp.broadcast_to(spread, (tensors, 128))
        upper = spread.astype(jnp.bfloat16)
        fac[0:tensors, :] = upper
        fac[tensors:lanes, :] = (spread - upper.astype(jnp.float32)).astype(jnp.bfloat16)
        table = fac[...]

    with scope("ag_core"):
        came(ga.at[column, 1 - c], gc_col)
        came(xs, gc_recv)

    with scope("apply"):
        step = 2
        for b in range(0, nq, step):
            spread = jnp.dot(
                hot[pl.ds(b * nc * rows, step * nc * rows), :], table, preferred_element_type=jnp.float32
            ).reshape(step, nc, rows, 128)
            part = pl.ds(b, step)
            newp[part] = pv[part] - (LR_OUTER * (1.0 + MU_OUTER)) * (ga[part] * spread)
        row0 = pl.multiple_of((mine * nc + c) * rows, rows)
        spread = jnp.dot(hot[pl.ds(row0, rows), :], table, preferred_element_type=jnp.float32)
        newm[...] = MU_OUTER * gm[mine, c] + ga[mine, c] * spread

    with scope("drain"):
        sent(xs, gx_send)
        sent(sib, gc_send)
        sent(xs, mx_send)
        sent(sib, mc_send)
        sent(all_of(sq2, nh * nq - 1), q_send.at[1])


def write_out(newp, newm, out_p, out_m, sem):
    copies = [pltpu.make_async_copy(newp, out_p, sem.at[0]), pltpu.make_async_copy(newm, out_m, sem.at[1])]
    for copy in copies:
        copy.start()
    for copy in copies:
        copy.wait()


VMEM_LIMIT = 52 * 1024 * 1024


def on_device(sizes, outer_delta, offsets, parameters, momentum):
    nx, nz, nc, ny, nh = (sizes[a] for a in AXES)
    rows = momentum.shape[0] // 128
    nq = nx * nz
    whole = (nq, nc, rows, 128)
    block = (rows, 128)
    f32 = jnp.float32
    dma = lambda *n: pltpu.SemaphoreType.DMA(n)
    vmem = pltpu.VMEM
    tensors = offsets.shape[0] - 1
    outs = (jax.ShapeDtypeStruct(whole, f32), jax.ShapeDtypeStruct(block, f32))
    in_vmem = (pl.BlockSpec(memory_space=pltpu.VMEM),) * 2
    results = pl.pallas_call(
        functools.partial(step_kernel, sizes),
        out_shape=outs,
        in_specs=[pl.BlockSpec(memory_space=pltpu.HBM)] * 4,
        out_specs=in_vmem,
        scratch_shapes=[
            vmem(whole, f32),
            vmem((nq,) + block, f32),
            vmem((nz,) + block, f32),
            vmem((nz,) + block, f32),
            vmem((nz,) + block, f32),
            vmem((nz - 2,) + block, f32),
            vmem(block, f32),
            vmem(whole, f32),
            vmem(whole, f32),
            vmem(whole, f32),
            vmem((1, tensors + 1), jnp.int32),
            vmem((nq * nc * rows, 2 * tensors), jnp.bfloat16),
            vmem((2 * tensors, 128), jnp.bfloat16),
            vmem((ny * nc, 1, 2 * tensors), f32),
            vmem((nh * nq, 1, 2 * tensors), f32),
            dma(5),
            dma(), dma(nz), dma(),
            dma(), dma(nz),
            dma(), dma(), dma(), dma(),
            dma(), dma(nz - 1), dma(), dma(nz), dma(), dma(), dma(),
            dma(), dma(), dma(), dma(2), dma(), dma(),
            dma(2), dma(2), pltpu.SemaphoreType.REGULAR((nz - 1,)), pltpu.SemaphoreType.REGULAR,
        ],
        compiler_params=pltpu.CompilerParams(
            collective_id=0, has_side_effects=True, vmem_limit_bytes=VMEM_LIMIT
        ),
    )(
        outer_delta.reshape(whole),
        momentum.reshape(block),
        parameters.reshape(whole),
        offsets.reshape(1, tensors + 1),
    )
    new_parameters, new_momentum = pl.pallas_call(
        write_out,
        out_shape=outs,
        in_specs=list(in_vmem),
        out_specs=(pl.BlockSpec(memory_space=pl.ANY),) * 2,
        scratch_shapes=[dma(2)],
        compiler_params=pltpu.CompilerParams(vmem_limit_bytes=4 * 1024 * 1024),
    )(*results)
    return new_parameters.reshape(parameters.shape), new_momentum.reshape(momentum.shape)


def solution(mesh):
    finer = Mesh(mesh.devices.reshape(2, 8, 2, 8, 2), AXES)
    sizes = dict(finer.shape)
    return jax.shard_map(
        functools.partial(on_device, sizes),
        mesh=finer,
        in_specs=(P(REP, SHARD), P(), P(SHARD), P(SHARD_REP)),
        out_specs=(P(SHARD), P(SHARD_REP)),
        check_vma=False,
    )
```

```python
import functools

import jax
import jax.numpy as jnp
from jax import lax
from jax.experimental import pallas as pl
from jax.experimental.pallas import tpu as pltpu
from jax.sharding import Mesh
from jax.sharding import PartitionSpec as P

X, Z, CORE, Y, XH = "rep_0", "rep_1", "rep_2", "shard_0", "shard_1"
AXES = (X, Z, CORE, Y, XH)
REP = (X, Z, CORE)
SHARD = (Y, XH)
SHARD_REP = (Y, XH, X, Z, CORE)

LR_OUTER = 0.7
MU_OUTER = 0.9
CLIP_RMS = 0.1
EPSILON = 1e-06


def remote(src, dst, send, recv, dev):
    return pltpu.make_async_remote_copy(
        src_ref=src,
        dst_ref=dst,
        send_sem=send,
        recv_sem=recv,
        device_id=dev,
        device_id_type=pl.DeviceIdType.MESH,
    )


def rs_order(half):
    order = [half]
    for d in range(half - 1, 0, -1):
        order += [-d, d]
    if half > 2:
        order.remove(half - 1)
        order.insert(half, half - 1)
    return order + [0]


def step_kernel(
    sizes,
    delta, mom, par, offs,
    newp, newm,
    dl, sib, xs, xr, zs, zr, ar, ga, gm, pv, ov, hot, fac, sq1, sq2,
    lsem, c_send, c_far, c_near, x_send, x_recv, z_send, z_recv, a_send, a_recv,
    gz_send, gz_recv, gx_send, gx_recv, gc_send, gc_col, gc_recv,
    mx_send, mx_recv, mz_send, mz_recv, mc_send, mc_recv, q_send, q_recv, in_column, in_peers,
):
    nx, nz, nc, ny, nh = (sizes[a] for a in AXES)
    x, z, c, y, h = (lax.axis_index(a) for a in AXES)
    rows = xs.shape[1]
    nq, half = nx * nz, nz // 2
    scope = jax.named_scope
    s = 1 - 2 * c
    zof = lambda d: lax.rem(z + s * d + nz, nz)
    mine, near, away = x * nz + z, x * nz, (1 - x) * nz
    column = pl.ds(near, nz)
    x_nb, c_nb = {X: 1 - x}, {CORE: 1 - c}
    z_dev = lambda d: {Z: zof(d)}

    barrier = pltpu.get_barrier_semaphore()
    peers1 = [
        {Y: lax.rem(y + a, ny), CORE: lax.rem(c + b, nc)}
        for a in range(ny) for b in range(nc) if a or b
    ]
    peers2 = [
        {XH: lax.rem(h + a, nh), X: lax.rem(x + b, nx), Z: lax.rem(z + e, nz)}
        for a in range(nh) for b in range(nx) for e in range(nz) if a or b or e
    ]
    row = [
        {XH: lax.rem(h + a, nh), X: lax.rem(x + b, nx)}
        for a in range(nh) for b in range(nx) if a or b
    ]
    pair = [{X: b} for b in range(nx)]
    cores = [{CORE: e} for e in range(nc)]

    def tell(sem, dev):
        pl.semaphore_signal(sem, inc=1, device_id=dev, device_id_type=pl.DeviceIdType.MESH)

    def tell_each(sem, axis, first, last, devs):
        def at(i, carry):
            for dev in devs:
                tell(sem, dev | {axis: i})
            return carry

        lax.fori_loop(first, last, at, 0)

    def wait_for(sem, count):
        @pl.when(count > 0)
        def _():
            pl.semaphore_wait(sem, count)

    load_m = pltpu.make_async_copy(mom, gm.at[mine, c], lsem.at[0])
    load_m.start()
    load_away = pltpu.make_async_copy(delta.at[:, pl.ds(1 - c, 1)], dl.at[:, pl.ds(1 - c, 1)], lsem.at[1])
    load_away.start()
    load_own = pltpu.make_async_copy(delta.at[:, pl.ds(c, 1)], dl.at[:, pl.ds(c, 1)], lsem.at[2])
    load_own.start()
    with scope("signal"):
        for dev in (c_nb, x_nb):
            tell(barrier, dev)
        tell_each(barrier, XH, h + 1, nh, pair)
        tell_each(barrier, Z, z + 1, nz, [{}] + row)
        tell_each(barrier, Y, y + 1, ny, cores)
    load_o = pltpu.make_async_copy(offs, ov, lsem.at[3])
    load_o.start()
    load_p = pltpu.make_async_copy(par, pv, lsem.at[4])
    load_p.start()
    with scope("load"):
        load_m.wait()
        load_away.wait()
    with scope("barrier"):
        pl.semaphore_wait(barrier, 2 + h * nx + y * nc + z * (1 + len(row)))

        def tell_column(i, carry):
            tell(in_column.at[z - 1 - i], {Z: i})
            return carry

        lax.fori_loop(0, z, tell_column, 0)

    def send(src, dst, send_sem, recv_sem, dev):
        remote(src, dst, send_sem, recv_sem, dev).start()

    def sent(ref, send_sem):
        remote(ref, ref, send_sem, send_sem, c_nb).wait_send()

    def came(ref, recv_sem):
        remote(ref, ref, recv_sem, recv_sem, c_nb).wait_recv()

    def all_of(ref, count):
        return ref.at[pl.ds(0, count)]

    own_m = gm.at[mine, c]
    near_m = [e * d for d in range(1, max(half - 1, 2)) for e in (1, -1)]
    last = near_m[-2]
    passed = [(-last, 1), (-last, 2), (last, -1)] if half > 2 else [(-last, 1)]
    send(own_m, own_m, mx_send, mx_recv, x_nb)
    reach = max(near_m)

    def momentum_to(i, condition):
        @pl.when(condition)
        def _():
            send(own_m, own_m, mz_send, mz_recv.at[0], {Z: i})

    def momentum_across(d):
        blk = gm.at[near + zof(d), c]
        send(blk, blk, mx_send, mx_recv, x_nb)

    def momentum_near():
        came(all_of(xs, len(near_m)), mz_recv.at[0])
        for d, to in passed:
            blk = gm.at[near + zof(d), c]
            send(blk, blk, mz_send, mz_recv.at[1], z_dev(to))
        for d in near_m:
            momentum_across(-d)

    def momentum_far():
        came(all_of(xs, len(passed)), mz_recv.at[1])
        for d, to in passed:
            momentum_across(d - to)
        send(gm.at[column, c], gm.at[column, c], mc_send, mc_recv, c_nb)

    steps = rs_order(half)
    with scope("core_send"):
        for i in range(nz):
            q = away + zof(-steps[i])
            send(dl.at[q, 1 - c], sib.at[q], c_send, c_far.at[i], c_nb)
        send(dl.at[column, 1 - c], sib.at[column], c_send, c_near, c_nb)
        load_own.wait()

    with scope("m_smaller"):
        for d in near_m:
            momentum_to(zof(d), zof(d) < z)
    with scope("tell"):
        tell_each(in_peers, XH, 0, h, pair)
        tell_each(in_peers, Z, 0, z, row)
        tell_each(in_peers, Y, 0, y, cores)
    with scope("x_stage"):
        for i in range(nz):
            q = away + zof(steps[i])
            came(sib.at[q], c_far.at[i])
            xs[i] = dl[q, c] + sib[q]
            send(xs.at[i], xr.at[i], x_send, x_recv.at[i], x_nb)

    own_len = rows * 128
    shard_pos = (y * nh + h) * (nq * nc * own_len)
    tensors = ov.shape[1] - 1
    with scope("one_hot"):
        load_o.wait()
        low, high = ov[:, 0:tensors], ov[:, 1 : tensors + 1]
        low, high = jnp.concatenate([low, low], axis=1), jnp.concatenate([high, high], axis=1)
        lanes = 2 * tensors

        def row_mask(first_pos):
            pos = first_pos + 128 * lax.broadcasted_iota(jnp.int32, (rows, lanes), 0)
            return (pos >= low) & (pos < high)

        for b in range(nq * nc):
            inside = row_mask(shard_pos + b * own_len)
            hot[pl.ds(b * rows, rows), :] = jnp.where(inside, 1.0, 0.0).astype(jnp.bfloat16)

    with scope("column"):
        for e in range(1, nz):
            @pl.when(z + e < nz)
            def _(e=e):
                pl.semaphore_wait(in_column.at[e - 1], 1)

            if e <= reach:
                momentum_to(z + e, z + e < nz)
        for e in range(1, reach + 1):
            momentum_to(z - e + nz, z - e < 0)
    came(sib.at[column], c_near)

    def carrier(i, condition):
        @pl.when(condition)
        def _():
            came(ar, a_recv)
            zs[i] = zs[i] + ar[...]
            send(zs.at[i], zr.at[i - 1], z_send, z_recv, z_dev(half - 1))

    for i in range(nz):
        d = steps[i]
        with scope(f"z_stage{i}"):
            q = near + zof(d)
            came(xr.at[i], x_recv.at[i])
            part = dl[q, c] + sib[q] + xr[i]
            zs[i] = part
            if i == 0:
                send(zs.at[i], ar, a_send, a_recv, z_dev(1))
            elif d == half - 1:
                carrier(i, 2 * z >= nz)
            elif d != 0:
                send(zs.at[i], zr.at[i - 1], z_send, z_recv, z_dev(d))
    with scope("carrier"):
        carrier(steps.index(half - 1), 2 * z < nz)
    with scope("m_near"):
        momentum_near()

    with scope("z_sum"):
        came(zr, z_recv)
        total = zs[nz - 1]
        for i in range(nz - 2):
            total = total + zr[i]
        avg = total * (1.0 / (nq * nc))
        ga[mine, c] = avg

    slot1 = y * nc + c
    with scope("squares"):
        squares = jnp.sum(avg * avg, axis=1, keepdims=True)
        mask = row_mask(shard_pos + (mine * nc + c) * own_len)
        sq1[slot1] = jnp.sum(jnp.where(mask, squares, 0.0), axis=0, keepdims=True)
        wait_for(in_peers, (nh - 1 - h) * nx + (ny - 1 - y) * nc + (nz - 1 - z) * len(row))
        for dev in peers1:
            send(sq1.at[slot1], sq1.at[slot1], q_send.at[0], q_recv.at[0], dev)

    own = ga.at[mine, c]
    hops = [e * d for d in list(range(2, half)) + [1] for e in (1, -1)]
    relay = -min(2, half - 1)
    from_z = [-d for d in hops] + [-half]
    origins = from_z + [0]
    beyond = [i for i in range(2, nz - 2) if abs(from_z[i]) > 1]
    beside = [i for i in range(2, nz - 2) if abs(from_z[i]) == 1]
    with scope("ag_send"):
        for i, d in enumerate(hops):
            if i in beside:
                continue
            send(own, own, gz_send, gz_recv.at[i], z_dev(d))
        send(own, own, gx_send, gx_recv.at[nz - 1], x_nb)

    def mean_from_z(i):
        blk = ga.at[near + zof(from_z[i]), c]
        came(blk, gz_recv.at[i])
        if from_z[i] == relay:
            send(blk, blk, gz_send, gz_recv.at[nz - 2], z_dev(half + relay))
        if abs(from_z[i]) > 1:
            send(blk, blk, gx_send, gx_recv.at[i], x_nb)

    def mean_beside():
        across = ga.at[away + z, c]
        for k, d in enumerate(from_z):
            if abs(d) == 1:
                if k in beside:
                    send(own, own, gz_send, gz_recv.at[k], z_dev(-d))
                send(across, across, gx_send, gx_recv.at[k], z_dev(-d))

    def mean_from_x(i):
        blk = ga.at[away + zof(origins[i]), c]
        came(blk, gx_recv.at[i])
        if origins[i] == 0 and half == 2:
            mean_beside()
        send(blk, blk, gc_send, gc_recv, c_nb)

    slot2 = (h * nx + x) * nz + z

    def exchange_squares(condition):
        @pl.when(condition)
        def _():
            with scope("q1"):
                came(all_of(sq1, ny * nc - 1), q_recv.at[0])
                acc = sq1[0]
                for i in range(1, ny * nc):
                    acc = acc + sq1[i]
                sq2[slot2] = acc
                for dev in peers2:
                    send(sq2.at[slot2], sq2.at[slot2], q_send.at[1], q_recv.at[1], dev)

    with scope("m_far"):
        momentum_far()
    with scope("ag_x_own"):
        mean_from_x(nz - 1)
    exchange_squares(2 * y >= ny)
    if half > 2:
        mean_beside()
    for i in [0, 1] + beyond:
        with scope(f"ag_z{i}"):
            mean_from_z(i)

    exchange_squares(2 * y < ny)
    for i in [nz - 2] + beside:
        with scope(f"ag_z{i}"):
            mean_from_z(i)
    send(ga.at[column, c], ga.at[column, c], gc_send, gc_col, c_nb)
    with scope("m_x"):
        other = gm.at[pl.ds(away, nz), c]
        came(other, mx_recv)
        send(other, other, mc_send, mc_recv, c_nb)
    with scope("drain1"):
        sent(sib, c_send)
        sent(xs, x_send)
        sent(zr, z_send)
        sent(ar, a_send)
        sent(all_of(xs, nz - 1), gz_send)
        sent(all_of(xs, nz - 1), mz_send)
        sent(all_of(sq1, ny * nc - 1), q_send.at[0])
    for i in [0, 1] + beside:
        with scope(f"ag_x{i}"):
            mean_from_x(i)
    for i in beyond:
        with scope(f"ag_x{i}"):
            mean_from_x(i)

    with scope("m_core"):
        came(gm.at[:, 1 - c], mc_recv)
    with scope("base"):
        load_p.wait()
        for q in range(nq):
            pv[q] = pv[q] - (LR_OUTER * MU_OUTER * MU_OUTER) * gm[q]
    with scope("ag_x_far"):
        mean_from_x(nz - 2)

    with scope("q2"):
        came(all_of(sq2, nh * nq - 1), q_recv.at[1])
        acc = sq2[0]
        for i in range(1, nh * nq):
            acc = acc + sq2[i]
    with scope("factor"):
        lengths = (high - low).astype(jnp.float32)
        factor = jnp.minimum(1.0, CLIP_RMS * jnp.sqrt(lengths) * lax.rsqrt(acc + EPSILON))
        at = lambda axis: lax.broadcasted_iota(jnp.int32, (tensors, lanes), axis)
        spread = jnp.sum(jnp.where(at(0) == at(1), factor, 0.0), axis=1, keepdims=True)
        spread = jnp.broadcast_to(spread, (tensors, 128))
        upper = spread.astype(jnp.bfloat16)
        fac[0:tensors, :] = upper
        fac[tensors:lanes, :] = (spread - upper.astype(jnp.float32)).astype(jnp.bfloat16)
        table = fac[...]

    with scope("ag_core"):
        came(ga.at[column, 1 - c], gc_col)
        came(xs, gc_recv)

    with scope("apply"):
        step = 2
        for b in range(0, nq, step):
            spread = jnp.dot(
                hot[pl.ds(b * nc * rows, step * nc * rows), :], table, preferred_element_type=jnp.float32
            ).reshape(step, nc, rows, 128)
            part = pl.ds(b, step)
            newp[part] = pv[part] - (LR_OUTER * (1.0 + MU_OUTER)) * (ga[part] * spread)
        row0 = pl.multiple_of((mine * nc + c) * rows, rows)
        spread = jnp.dot(hot[pl.ds(row0, rows), :], table, preferred_element_type=jnp.float32)
        newm[...] = MU_OUTER * gm[mine, c] + ga[mine, c] * spread

    with scope("drain"):
        sent(xs, gx_send)
        sent(sib, gc_send)
        sent(xs, mx_send)
        sent(sib, mc_send)
        sent(all_of(sq2, nh * nq - 1), q_send.at[1])


def write_out(newp, newm, out_p, out_m, sem):
    copies = [pltpu.make_async_copy(newp, out_p, sem.at[0]), pltpu.make_async_copy(newm, out_m, sem.at[1])]
    for copy in copies:
        copy.start()
    for copy in copies:
        copy.wait()


VMEM_LIMIT = 52 * 1024 * 1024


def on_device(sizes, outer_delta, offsets, parameters, momentum):
    nx, nz, nc, ny, nh = (sizes[a] for a in AXES)
    rows = momentum.shape[0] // 128
    nq = nx * nz
    whole = (nq, nc, rows, 128)
    block = (rows, 128)
    f32 = jnp.float32
    dma = lambda *n: pltpu.SemaphoreType.DMA(n)
    vmem = pltpu.VMEM
    tensors = offsets.shape[0] - 1
    outs = (jax.ShapeDtypeStruct(whole, f32), jax.ShapeDtypeStruct(block, f32))
    in_vmem = (pl.BlockSpec(memory_space=pltpu.VMEM),) * 2
    results = pl.pallas_call(
        functools.partial(step_kernel, sizes),
        out_shape=outs,
        in_specs=[pl.BlockSpec(memory_space=pltpu.HBM)] * 4,
        out_specs=in_vmem,
        scratch_shapes=[
            vmem(whole, f32),
            vmem((nq,) + block, f32),
            vmem((nz,) + block, f32),
            vmem((nz,) + block, f32),
            vmem((nz,) + block, f32),
            vmem((nz - 2,) + block, f32),
            vmem(block, f32),
            vmem(whole, f32),
            vmem(whole, f32),
            vmem(whole, f32),
            vmem((1, tensors + 1), jnp.int32),
            vmem((nq * nc * rows, 2 * tensors), jnp.bfloat16),
            vmem((2 * tensors, 128), jnp.bfloat16),
            vmem((ny * nc, 1, 2 * tensors), f32),
            vmem((nh * nq, 1, 2 * tensors), f32),
            dma(5),
            dma(), dma(nz), dma(),
            dma(), dma(nz),
            dma(), dma(), dma(), dma(),
            dma(), dma(nz - 1), dma(), dma(nz), dma(), dma(), dma(),
            dma(), dma(), dma(), dma(2), dma(), dma(),
            dma(2), dma(2), pltpu.SemaphoreType.REGULAR((nz - 1,)), pltpu.SemaphoreType.REGULAR,
        ],
        compiler_params=pltpu.CompilerParams(
            collective_id=0, has_side_effects=True, vmem_limit_bytes=VMEM_LIMIT
        ),
    )(
        outer_delta.reshape(whole),
        momentum.reshape(block),
        parameters.reshape(whole),
        offsets.reshape(1, tensors + 1),
    )
    new_parameters, new_momentum = pl.pallas_call(
        write_out,
        out_shape=outs,
        in_specs=list(in_vmem),
        out_specs=(pl.BlockSpec(memory_space=pl.ANY),) * 2,
        scratch_shapes=[dma(2)],
        compiler_params=pltpu.CompilerParams(vmem_limit_bytes=4 * 1024 * 1024),
    )(*results)
    return new_parameters.reshape(parameters.shape), new_momentum.reshape(momentum.shape)


def solution(mesh):
    finer = Mesh(mesh.devices.reshape(2, 8, 2, 8, 2), AXES)
    sizes = dict(finer.shape)
    return jax.shard_map(
        functools.partial(on_device, sizes),
        mesh=finer,
        in_specs=(P(REP, SHARD), P(), P(SHARD), P(SHARD_REP)),
        out_specs=(P(SHARD), P(SHARD_REP)),
        check_vma=False,
    )
```

```python
import functools

import jax
import jax.numpy as jnp
from jax import lax
from jax.experimental import pallas as pl
from jax.experimental.pallas import tpu as pltpu
from jax.sharding import Mesh
from jax.sharding import PartitionSpec as P

X, Z, CORE, Y, XH = "rep_0", "rep_1", "rep_2", "shard_0", "shard_1"
AXES = (X, Z, CORE, Y, XH)
REP = (X, Z, CORE)
SHARD = (Y, XH)
SHARD_REP = (Y, XH, X, Z, CORE)

LR_OUTER = 0.7
MU_OUTER = 0.9
CLIP_RMS = 0.1
EPSILON = 1e-06


def remote(src, dst, send, recv, dev):
    return pltpu.make_async_remote_copy(
        src_ref=src,
        dst_ref=dst,
        send_sem=send,
        recv_sem=recv,
        device_id=dev,
        device_id_type=pl.DeviceIdType.MESH,
    )


def rs_order(half):
    order = [half]
    for d in range(half - 1, 0, -1):
        order += [-d, d]
    if half > 2:
        order.remove(half - 1)
        order.insert(half, half - 1)
    return order + [0]


def step_kernel(
    sizes,
    delta, mom, par, offs,
    newp, newm,
    dl, sib, xs, xr, zs, zr, ar, ga, gm, pv, ov, hot, fac, sq1, sq2,
    lsem, c_send, c_far, c_near, x_send, x_recv, z_send, z_recv, a_send, a_recv,
    gz_send, gz_recv, gx_send, gx_recv, gc_send, gc_col, gc_recv,
    mx_send, mx_recv, mz_send, mz_recv, mc_send, mc_recv, q_send, q_recv, in_column, in_peers,
):
    nx, nz, nc, ny, nh = (sizes[a] for a in AXES)
    x, z, c, y, h = (lax.axis_index(a) for a in AXES)
    rows = xs.shape[1]
    nq, half = nx * nz, nz // 2
    scope = jax.named_scope
    s = 1 - 2 * c
    zof = lambda d: lax.rem(z + s * d + nz, nz)
    mine, near, away = x * nz + z, x * nz, (1 - x) * nz
    column = pl.ds(near, nz)
    x_nb, c_nb = {X: 1 - x}, {CORE: 1 - c}
    z_dev = lambda d: {Z: zof(d)}

    barrier = pltpu.get_barrier_semaphore()
    peers1 = [
        {Y: lax.rem(y + a, ny), CORE: lax.rem(c + b, nc)}
        for a in range(ny) for b in range(nc) if a or b
    ]
    peers2 = [
        {XH: lax.rem(h + a, nh), X: lax.rem(x + b, nx), Z: lax.rem(z + e, nz)}
        for a in range(nh) for b in range(nx) for e in range(nz) if a or b or e
    ]
    row = [
        {XH: lax.rem(h + a, nh), X: lax.rem(x + b, nx)}
        for a in range(nh) for b in range(nx) if a or b
    ]
    pair = [{X: b} for b in range(nx)]
    cores = [{CORE: e} for e in range(nc)]

    def tell(sem, dev):
        pl.semaphore_signal(sem, inc=1, device_id=dev, device_id_type=pl.DeviceIdType.MESH)

    def tell_each(sem, axis, first, last, devs):
        def at(i, carry):
            for dev in devs:
                tell(sem, dev | {axis: i})
            return carry

        lax.fori_loop(first, last, at, 0)

    def wait_for(sem, count):
        @pl.when(count > 0)
        def _():
            pl.semaphore_wait(sem, count)

    load_m = pltpu.make_async_copy(mom, gm.at[mine, c], lsem.at[0])
    load_m.start()
    load_away = pltpu.make_async_copy(delta.at[:, pl.ds(1 - c, 1)], dl.at[:, pl.ds(1 - c, 1)], lsem.at[1])
    load_away.start()
    load_own = pltpu.make_async_copy(delta.at[:, pl.ds(c, 1)], dl.at[:, pl.ds(c, 1)], lsem.at[2])
    load_own.start()
    with scope("signal"):
        for dev in (c_nb, x_nb):
            tell(barrier, dev)
        tell_each(barrier, XH, h + 1, nh, pair)
        tell_each(barrier, Z, z + 1, nz, [{}] + row)
        tell_each(barrier, Y, y + 1, ny, cores)
    load_o = pltpu.make_async_copy(offs, ov, lsem.at[3])
    load_o.start()
    load_p = pltpu.make_async_copy(par, pv, lsem.at[4])
    load_p.start()
    with scope("load"):
        load_m.wait()
        load_away.wait()
    with scope("barrier"):
        pl.semaphore_wait(barrier, 2 + h * nx + y * nc + z * (1 + len(row)))

        def tell_column(i, carry):
            tell(in_column.at[z - 1 - i], {Z: i})
            return carry

        lax.fori_loop(0, z, tell_column, 0)

    def send(src, dst, send_sem, recv_sem, dev):
        remote(src, dst, send_sem, recv_sem, dev).start()

    def sent(ref, send_sem):
        remote(ref, ref, send_sem, send_sem, c_nb).wait_send()

    def came(ref, recv_sem):
        remote(ref, ref, recv_sem, recv_sem, c_nb).wait_recv()

    def all_of(ref, count):
        return ref.at[pl.ds(0, count)]

    own_m = gm.at[mine, c]
    near_m = [e * d for d in range(1, max(half - 1, 2)) for e in (1, -1)]
    last = near_m[-2]
    passed = [(-last, 1), (-last, 2), (last, -1)] if half > 2 else [(-last, 1)]
    send(own_m, own_m, mx_send, mx_recv, x_nb)
    reach = max(near_m)

    def momentum_to(i, condition):
        @pl.when(condition)
        def _():
            send(own_m, own_m, mz_send, mz_recv.at[0], {Z: i})

    def momentum_across(d):
        blk = gm.at[near + zof(d), c]
        send(blk, blk, mx_send, mx_recv, x_nb)

    def momentum_near():
        came(all_of(xs, len(near_m)), mz_recv.at[0])
        for d, to in passed:
            blk = gm.at[near + zof(d), c]
            send(blk, blk, mz_send, mz_recv.at[1], z_dev(to))
        for d in near_m:
            momentum_across(-d)

    def momentum_far():
        came(all_of(xs, len(passed)), mz_recv.at[1])
        for d, to in passed:
            momentum_across(d - to)
        send(gm.at[column, c], gm.at[column, c], mc_send, mc_recv, c_nb)

    steps = rs_order(half)
    with scope("core_send"):
        for i in range(nz):
            q = away + zof(-steps[i])
            send(dl.at[q, 1 - c], sib.at[q], c_send, c_far.at[i], c_nb)
        send(dl.at[column, 1 - c], sib.at[column], c_send, c_near, c_nb)
        load_own.wait()

    with scope("m_smaller"):
        for d in near_m:
            momentum_to(zof(d), zof(d) < z)
    with scope("tell"):
        tell_each(in_peers, XH, 0, h, pair)
        tell_each(in_peers, Z, 0, z, row)
        tell_each(in_peers, Y, 0, y, cores)
    with scope("x_stage"):
        for i in range(nz):
            q = away + zof(steps[i])
            came(sib.at[q], c_far.at[i])
            xs[i] = dl[q, c] + sib[q]
            send(xs.at[i], xr.at[i], x_send, x_recv.at[i], x_nb)

    own_len = rows * 128
    shard_pos = (y * nh + h) * (nq * nc * own_len)
    tensors = ov.shape[1] - 1
    with scope("one_hot"):
        load_o.wait()
        low, high = ov[:, 0:tensors], ov[:, 1 : tensors + 1]
        low, high = jnp.concatenate([low, low], axis=1), jnp.concatenate([high, high], axis=1)
        lanes = 2 * tensors

        def row_mask(first_pos):
            pos = first_pos + 128 * lax.broadcasted_iota(jnp.int32, (rows, lanes), 0)
            return (pos >= low) & (pos < high)

        for b in range(nq * nc):
            inside = row_mask(shard_pos + b * own_len)
            hot[pl.ds(b * rows, rows), :] = jnp.where(inside, 1.0, 0.0).astype(jnp.bfloat16)

    with scope("column"):
        for e in range(1, nz):
            @pl.when(z + e < nz)
            def _(e=e):
                pl.semaphore_wait(in_column.at[e - 1], 1)

            if e <= reach:
                momentum_to(z + e, z + e < nz)
        for e in range(1, reach + 1):
            momentum_to(z - e + nz, z - e < 0)
    came(sib.at[column], c_near)

    def carrier(i, condition):
        @pl.when(condition)
        def _():
            came(ar, a_recv)
            zs[i] = zs[i] + ar[...]
            send(zs.at[i], zr.at[i - 1], z_send, z_recv, z_dev(half - 1))

    for i in range(nz):
        d = steps[i]
        with scope(f"z_stage{i}"):
            q = near + zof(d)
            came(xr.at[i], x_recv.at[i])
            part = dl[q, c] + sib[q] + xr[i]
            zs[i] = part
            if i == 0:
                send(zs.at[i], ar, a_send, a_recv, z_dev(1))
            elif d == half - 1:
                carrier(i, 2 * z >= nz)
            elif d != 0:
                send(zs.at[i], zr.at[i - 1], z_send, z_recv, z_dev(d))
    with scope("carrier"):
        carrier(steps.index(half - 1), 2 * z < nz)
    with scope("m_near"):
        momentum_near()

    with scope("z_sum"):
        came(zr, z_recv)
        total = zs[nz - 1]
        for i in range(nz - 2):
            total = total + zr[i]
        avg = total * (1.0 / (nq * nc))
        ga[mine, c] = avg

    slot1 = y * nc + c
    with scope("squares"):
        squares = jnp.sum(avg * avg, axis=1, keepdims=True)
        mask = row_mask(shard_pos + (mine * nc + c) * own_len)
        sq1[slot1] = jnp.sum(jnp.where(mask, squares, 0.0), axis=0, keepdims=True)
        wait_for(in_peers, (nh - 1 - h) * nx + (ny - 1 - y) * nc + (nz - 1 - z) * len(row))
        for dev in peers1:
            send(sq1.at[slot1], sq1.at[slot1], q_send.at[0], q_recv.at[0], dev)

    own = ga.at[mine, c]
    hops = [e * d for d in list(range(2, half)) + [1] for e in (1, -1)]
    relay = -min(2, half - 1)
    from_z = [-d for d in hops] + [-half]
    origins = from_z + [0]
    beyond = [i for i in range(2, nz - 2) if abs(from_z[i]) > 1]
    beside = [i for i in range(2, nz - 2) if abs(from_z[i]) == 1]
    with scope("ag_send"):
        for i, d in enumerate(hops):
            if i in beside:
                continue
            send(own, own, gz_send, gz_recv.at[i], z_dev(d))
        send(own, own, gx_send, gx_recv.at[nz - 1], x_nb)

    def mean_from_z(i):
        blk = ga.at[near + zof(from_z[i]), c]
        came(blk, gz_recv.at[i])
        if from_z[i] == relay:
            send(blk, blk, gz_send, gz_recv.at[nz - 2], z_dev(half + relay))
        if abs(from_z[i]) > 1:
            send(blk, blk, gx_send, gx_recv.at[i], x_nb)
        if i == nz - 2:
            send(blk, blk, gc_send, gc_recv, {X: 1 - x, CORE: 1 - c})

    def mean_beside():
        across = ga.at[away + z, c]
        for k, d in enumerate(from_z):
            if abs(d) == 1:
                if k in beside:
                    send(own, own, gz_send, gz_recv.at[k], z_dev(-d))
                send(across, across, gx_send, gx_recv.at[k], z_dev(-d))

    def mean_from_x(i):
        blk = ga.at[away + zof(origins[i]), c]
        came(blk, gx_recv.at[i])
        if origins[i] == 0 and half == 2:
            mean_beside()
        if i != nz - 2:
            send(blk, blk, gc_send, gc_recv, c_nb)

    slot2 = (h * nx + x) * nz + z

    def exchange_squares(condition):
        @pl.when(condition)
        def _():
            with scope("q1"):
                came(all_of(sq1, ny * nc - 1), q_recv.at[0])
                acc = sq1[0]
                for i in range(1, ny * nc):
                    acc = acc + sq1[i]
                sq2[slot2] = acc
                for dev in peers2:
                    send(sq2.at[slot2], sq2.at[slot2], q_send.at[1], q_recv.at[1], dev)

    with scope("m_far"):
        momentum_far()
    with scope("ag_x_own"):
        mean_from_x(nz - 1)
    exchange_squares(2 * y >= ny)
    for i in [0, 1] + beyond:
        with scope(f"ag_z{i}"):
            mean_from_z(i)
        if i == 1 and half > 2:
            mean_beside()

    exchange_squares(2 * y < ny)
    for i in [nz - 2] + beside:
        with scope(f"ag_z{i}"):
            mean_from_z(i)
    send(ga.at[column, c], ga.at[column, c], gc_send, gc_col, c_nb)
    with scope("m_x"):
        other = gm.at[pl.ds(away, nz), c]
        came(other, mx_recv)
        send(other, other, mc_send, mc_recv, c_nb)
    with scope("drain1"):
        sent(sib, c_send)
        sent(xs, x_send)
        sent(zr, z_send)
        sent(ar, a_send)
        sent(all_of(xs, nz - 1), gz_send)
        sent(all_of(xs, nz - 1), mz_send)
        sent(all_of(sq1, ny * nc - 1), q_send.at[0])
    for i in [0, 1] + beside:
        with scope(f"ag_x{i}"):
            mean_from_x(i)
    for i in beyond:
        with scope(f"ag_x{i}"):
            mean_from_x(i)

    with scope("m_core"):
        came(gm.at[:, 1 - c], mc_recv)
    with scope("base"):
        load_p.wait()
        for q in range(nq):
            pv[q] = pv[q] - (LR_OUTER * MU_OUTER * MU_OUTER) * gm[q]
    with scope("ag_x_far"):
        mean_from_x(nz - 2)

    with scope("q2"):
        came(all_of(sq2, nh * nq - 1), q_recv.at[1])
        acc = sq2[0]
        for i in range(1, nh * nq):
            acc = acc + sq2[i]
    with scope("factor"):
        lengths = (high - low).astype(jnp.float32)
        factor = jnp.minimum(1.0, CLIP_RMS * jnp.sqrt(lengths) * lax.rsqrt(acc + EPSILON))
        at = lambda axis: lax.broadcasted_iota(jnp.int32, (tensors, lanes), axis)
        spread = jnp.sum(jnp.where(at(0) == at(1), factor, 0.0), axis=1, keepdims=True)
        spread = jnp.broadcast_to(spread, (tensors, 128))
        upper = spread.astype(jnp.bfloat16)
        fac[0:tensors, :] = upper
        fac[tensors:lanes, :] = (spread - upper.astype(jnp.float32)).astype(jnp.bfloat16)
        table = fac[...]

    with scope("ag_core"):
        came(ga.at[column, 1 - c], gc_col)
        came(xs, gc_recv)

    with scope("apply"):
        step = 2
        for b in range(0, nq, step):
            spread = jnp.dot(
                hot[pl.ds(b * nc * rows, step * nc * rows), :], table, preferred_element_type=jnp.float32
            ).reshape(step, nc, rows, 128)
            part = pl.ds(b, step)
            newp[part] = pv[part] - (LR_OUTER * (1.0 + MU_OUTER)) * (ga[part] * spread)
        row0 = pl.multiple_of((mine * nc + c) * rows, rows)
        spread = jnp.dot(hot[pl.ds(row0, rows), :], table, preferred_element_type=jnp.float32)
        newm[...] = MU_OUTER * gm[mine, c] + ga[mine, c] * spread

    with scope("drain"):
        sent(xs, gx_send)
        sent(sib, gc_send)
        sent(xs, mx_send)
        sent(sib, mc_send)
        sent(all_of(sq2, nh * nq - 1), q_send.at[1])


def write_out(newp, newm, out_p, out_m, sem):
    copies = [pltpu.make_async_copy(newp, out_p, sem.at[0]), pltpu.make_async_copy(newm, out_m, sem.at[1])]
    for copy in copies:
        copy.start()
    for copy in copies:
        copy.wait()


VMEM_LIMIT = 52 * 1024 * 1024


def on_device(sizes, outer_delta, offsets, parameters, momentum):
    nx, nz, nc, ny, nh = (sizes[a] for a in AXES)
    rows = momentum.shape[0] // 128
    nq = nx * nz
    whole = (nq, nc, rows, 128)
    block = (rows, 128)
    f32 = jnp.float32
    dma = lambda *n: pltpu.SemaphoreType.DMA(n)
    vmem = pltpu.VMEM
    tensors = offsets.shape[0] - 1
    outs = (jax.ShapeDtypeStruct(whole, f32), jax.ShapeDtypeStruct(block, f32))
    in_vmem = (pl.BlockSpec(memory_space=pltpu.VMEM),) * 2
    results = pl.pallas_call(
        functools.partial(step_kernel, sizes),
        out_shape=outs,
        in_specs=[pl.BlockSpec(memory_space=pltpu.HBM)] * 4,
        out_specs=in_vmem,
        scratch_shapes=[
            vmem(whole, f32),
            vmem((nq,) + block, f32),
            vmem((nz,) + block, f32),
            vmem((nz,) + block, f32),
            vmem((nz,) + block, f32),
            vmem((nz - 2,) + block, f32),
            vmem(block, f32),
            vmem(whole, f32),
            vmem(whole, f32),
            vmem(whole, f32),
            vmem((1, tensors + 1), jnp.int32),
            vmem((nq * nc * rows, 2 * tensors), jnp.bfloat16),
            vmem((2 * tensors, 128), jnp.bfloat16),
            vmem((ny * nc, 1, 2 * tensors), f32),
            vmem((nh * nq, 1, 2 * tensors), f32),
            dma(5),
            dma(), dma(nz), dma(),
            dma(), dma(nz),
            dma(), dma(), dma(), dma(),
            dma(), dma(nz - 1), dma(), dma(nz), dma(), dma(), dma(),
            dma(), dma(), dma(), dma(2), dma(), dma(),
            dma(2), dma(2), pltpu.SemaphoreType.REGULAR((nz - 1,)), pltpu.SemaphoreType.REGULAR,
        ],
        compiler_params=pltpu.CompilerParams(
            collective_id=0, has_side_effects=True, vmem_limit_bytes=VMEM_LIMIT
        ),
    )(
        outer_delta.reshape(whole),
        momentum.reshape(block),
        parameters.reshape(whole),
        offsets.reshape(1, tensors + 1),
    )
    new_parameters, new_momentum = pl.pallas_call(
        write_out,
        out_shape=outs,
        in_specs=list(in_vmem),
        out_specs=(pl.BlockSpec(memory_space=pl.ANY),) * 2,
        scratch_shapes=[dma(2)],
        compiler_params=pltpu.CompilerParams(vmem_limit_bytes=4 * 1024 * 1024),
    )(*results)
    return new_parameters.reshape(parameters.shape), new_momentum.reshape(momentum.shape)


def solution(mesh):
    finer = Mesh(mesh.devices.reshape(2, 8, 2, 8, 2), AXES)
    sizes = dict(finer.shape)
    return jax.shard_map(
        functools.partial(on_device, sizes),
        mesh=finer,
        in_specs=(P(REP, SHARD), P(), P(SHARD), P(SHARD_REP)),
        out_specs=(P(SHARD), P(SHARD_REP)),
        check_vma=False,
    )
```

```python
import functools

import jax
import jax.numpy as jnp
from jax import lax
from jax.experimental import pallas as pl
from jax.experimental.pallas import tpu as pltpu
from jax.sharding import Mesh
from jax.sharding import PartitionSpec as P

X, Z, CORE, Y, XH = "rep_0", "rep_1", "rep_2", "shard_0", "shard_1"
AXES = (X, Z, CORE, Y, XH)
REP = (X, Z, CORE)
SHARD = (Y, XH)
SHARD_REP = (Y, XH, X, Z, CORE)

LR_OUTER = 0.7
MU_OUTER = 0.9
CLIP_RMS = 0.1
EPSILON = 1e-06


def remote(src, dst, send, recv, dev):
    return pltpu.make_async_remote_copy(
        src_ref=src,
        dst_ref=dst,
        send_sem=send,
        recv_sem=recv,
        device_id=dev,
        device_id_type=pl.DeviceIdType.MESH,
    )


def rs_order(half):
    order = [half]
    for d in range(half - 1, 0, -1):
        order += [-d, d]
    if half > 2:
        order.remove(half - 1)
        order.insert(half, half - 1)
    return order + [0]


def in_pairs(terms):
    while len(terms) > 1:
        terms = [a + b for a, b in zip(terms[::2], terms[1::2])]
    return terms[0]


def step_kernel(
    sizes,
    delta, mom, par, offs,
    newp, newm,
    dl, sib, xs, xr, zs, zr, ar, ga, gm, pv, ov, hot, fac, sq1, sq2,
    lsem, c_send, c_far, c_near, x_send, x_recv, z_send, z_recv, a_send, a_recv,
    gz_send, gz_recv, gx_send, gx_recv, gc_send, gc_col, gc_recv,
    mx_send, mx_recv, mz_send, mz_recv, mc_send, mc_recv, q_send, q_recv, in_column, in_peers,
):
    nx, nz, nc, ny, nh = (sizes[a] for a in AXES)
    x, z, c, y, h = (lax.axis_index(a) for a in AXES)
    rows = xs.shape[1]
    nq, half = nx * nz, nz // 2
    scope = jax.named_scope
    s = 1 - 2 * c
    zof = lambda d: lax.rem(z + s * d + nz, nz)
    mine, near, away = x * nz + z, x * nz, (1 - x) * nz
    column = pl.ds(near, nz)
    x_nb, c_nb = {X: 1 - x}, {CORE: 1 - c}
    z_dev = lambda d: {Z: zof(d)}

    barrier = pltpu.get_barrier_semaphore()
    peers1 = [
        {Y: lax.rem(y + a, ny), CORE: lax.rem(c + b, nc)}
        for a in range(ny) for b in range(nc) if a or b
    ]
    peers2 = [
        {XH: lax.rem(h + a, nh), X: lax.rem(x + b, nx), Z: lax.rem(z + e, nz)}
        for a in range(nh) for b in range(nx) for e in range(nz) if a or b or e
    ]
    row = [
        {XH: lax.rem(h + a, nh), X: lax.rem(x + b, nx)}
        for a in range(nh) for b in range(nx) if a or b
    ]
    pair = [{X: b} for b in range(nx)]
    cores = [{CORE: e} for e in range(nc)]

    def tell(sem, dev):
        pl.semaphore_signal(sem, inc=1, device_id=dev, device_id_type=pl.DeviceIdType.MESH)

    def tell_each(sem, axis, first, last, devs):
        def at(i, carry):
            for dev in devs:
                tell(sem, dev | {axis: i})
            return carry

        lax.fori_loop(first, last, at, 0)

    def wait_for(sem, count):
        @pl.when(count > 0)
        def _():
            pl.semaphore_wait(sem, count)

    load_m = pltpu.make_async_copy(mom, gm.at[mine, c], lsem.at[0])
    load_m.start()
    load_away = pltpu.make_async_copy(delta.at[:, pl.ds(1 - c, 1)], dl.at[:, pl.ds(1 - c, 1)], lsem.at[1])
    load_away.start()
    load_own = pltpu.make_async_copy(delta.at[:, pl.ds(c, 1)], dl.at[:, pl.ds(c, 1)], lsem.at[2])
    load_own.start()
    with scope("signal"):
        for dev in (c_nb, x_nb):
            tell(barrier, dev)
        tell_each(barrier, XH, h + 1, nh, pair)
        tell_each(barrier, Z, z + 1, nz, [{}] + row)
        tell_each(barrier, Y, y + 1, ny, cores)
    load_o = pltpu.make_async_copy(offs, ov, lsem.at[3])
    load_o.start()
    load_p = pltpu.make_async_copy(par, pv, lsem.at[4])
    load_p.start()
    with scope("load"):
        load_m.wait()
        load_away.wait()
    with scope("barrier"):
        pl.semaphore_wait(barrier, 2 + h * nx + y * nc + z * (1 + len(row)))

        def tell_column(i, carry):
            tell(in_column.at[z - 1 - i], {Z: i})
            return carry

        lax.fori_loop(0, z, tell_column, 0)

    def send(src, dst, send_sem, recv_sem, dev):
        remote(src, dst, send_sem, recv_sem, dev).start()

    def sent(ref, send_sem):
        remote(ref, ref, send_sem, send_sem, c_nb).wait_send()

    def came(ref, recv_sem):
        remote(ref, ref, recv_sem, recv_sem, c_nb).wait_recv()

    def all_of(ref, count):
        return ref.at[pl.ds(0, count)]

    own_m = gm.at[mine, c]
    near_m = [e * d for d in range(1, max(half - 1, 2)) for e in (1, -1)]
    last = near_m[-2]
    passed = [(-last, 1), (-last, 2), (last, -1)] if half > 2 else [(-last, 1)]
    send(own_m, own_m, mx_send, mx_recv, x_nb)
    reach = max(near_m)

    def momentum_to(i, condition):
        @pl.when(condition)
        def _():
            send(own_m, own_m, mz_send, mz_recv.at[0], {Z: i})

    def momentum_across(d):
        blk = gm.at[near + zof(d), c]
        send(blk, blk, mx_send, mx_recv, x_nb)

    def momentum_near():
        came(all_of(xs, len(near_m)), mz_recv.at[0])
        for d, to in passed:
            blk = gm.at[near + zof(d), c]
            send(blk, blk, mz_send, mz_recv.at[1], z_dev(to))
        for d in near_m:
            momentum_across(-d)

    def momentum_far():
        came(all_of(xs, len(passed)), mz_recv.at[1])
        for d, to in passed:
            momentum_across(d - to)
        send(gm.at[column, c], gm.at[column, c], mc_send, mc_recv, c_nb)

    steps = rs_order(half)
    with scope("core_send"):
        for i in range(nz):
            q = away + zof(-steps[i])
            send(dl.at[q, 1 - c], sib.at[q], c_send, c_far.at[i], c_nb)
        send(dl.at[column, 1 - c], sib.at[column], c_send, c_near, c_nb)
        load_own.wait()

    with scope("m_smaller"):
        for d in near_m:
            momentum_to(zof(d), zof(d) < z)
    with scope("tell"):
        tell_each(in_peers, XH, 0, h, pair)
        tell_each(in_peers, Z, 0, z, row)
        tell_each(in_peers, Y, 0, y, cores)
    with scope("x_stage"):
        for i in range(nz):
            q = away + zof(steps[i])
            came(sib.at[q], c_far.at[i])
            xs[i] = dl[q, c] + sib[q]
            send(xs.at[i], xr.at[i], x_send, x_recv.at[i], x_nb)

    own_len = rows * 128
    shard_pos = (y * nh + h) * (nq * nc * own_len)
    tensors = ov.shape[1] - 1
    with scope("one_hot"):
        load_o.wait()
        low, high = ov[:, 0:tensors], ov[:, 1 : tensors + 1]
        low, high = jnp.concatenate([low, low], axis=1), jnp.concatenate([high, high], axis=1)
        lanes = 2 * tensors
        limit = CLIP_RMS * jnp.sqrt((high - low).astype(jnp.float32))

        def row_mask(first_pos):
            pos = first_pos + 128 * lax.broadcasted_iota(jnp.int32, (rows, lanes), 0)
            return (pos >= low) & (pos < high)

        for b in range(nq * nc):
            inside = row_mask(shard_pos + b * own_len)
            hot[pl.ds(b * rows, rows), :] = jnp.where(inside, 1.0, 0.0).astype(jnp.bfloat16)

    with scope("column"):
        for e in range(1, nz):
            @pl.when(z + e < nz)
            def _(e=e):
                pl.semaphore_wait(in_column.at[e - 1], 1)

            if e <= reach:
                momentum_to(z + e, z + e < nz)
        for e in range(1, reach + 1):
            momentum_to(z - e + nz, z - e < 0)
    came(sib.at[column], c_near)

    def carrier(i, condition):
        @pl.when(condition)
        def _():
            came(ar, a_recv)
            zs[i] = zs[i] + ar[...]
            send(zs.at[i], zr.at[i - 1], z_send, z_recv, z_dev(half - 1))

    for i in range(nz):
        d = steps[i]
        with scope(f"z_stage{i}"):
            q = near + zof(d)
            came(xr.at[i], x_recv.at[i])
            part = dl[q, c] + sib[q] + xr[i]
            zs[i] = part
            if i == 0:
                send(zs.at[i], ar, a_send, a_recv, z_dev(1))
            elif d == half - 1:
                carrier(i, 2 * z >= nz)
            elif d != 0:
                send(zs.at[i], zr.at[i - 1], z_send, z_recv, z_dev(d))
    with scope("carrier"):
        carrier(steps.index(half - 1), 2 * z < nz)
    with scope("m_near"):
        momentum_near()

    with scope("z_sum"):
        came(zr, z_recv)
        total = zs[nz - 1]
        for i in range(nz - 2):
            total = total + zr[i]
        avg = total * (1.0 / (nq * nc))
        ga[mine, c] = avg

    slot1 = y * nc + c
    with scope("squares"):
        squares = jnp.sum(avg * avg, axis=1, keepdims=True)
        mask = row_mask(shard_pos + (mine * nc + c) * own_len)
        sq1[slot1] = jnp.sum(jnp.where(mask, squares, 0.0), axis=0, keepdims=True)
        wait_for(in_peers, (nh - 1 - h) * nx + (ny - 1 - y) * nc + (nz - 1 - z) * len(row))
        for dev in peers1:
            send(sq1.at[slot1], sq1.at[slot1], q_send.at[0], q_recv.at[0], dev)

    own = ga.at[mine, c]
    hops = [e * d for d in list(range(2, half)) + [1] for e in (1, -1)]
    relay = -min(2, half - 1)
    from_z = [-d for d in hops] + [-half]
    origins = from_z + [0]
    beyond = [i for i in range(2, nz - 2) if abs(from_z[i]) > 1]
    beside = [i for i in range(2, nz - 2) if abs(from_z[i]) == 1]
    with scope("ag_send"):
        for i, d in enumerate(hops):
            if i in beside:
                continue
            send(own, own, gz_send, gz_recv.at[i], z_dev(d))
        send(own, own, gx_send, gx_recv.at[nz - 1], x_nb)

    def mean_from_z(i):
        blk = ga.at[near + zof(from_z[i]), c]
        came(blk, gz_recv.at[i])
        if from_z[i] == relay:
            send(blk, blk, gz_send, gz_recv.at[nz - 2], z_dev(half + relay))
        if abs(from_z[i]) > 1:
            send(blk, blk, gx_send, gx_recv.at[i], x_nb)
        if i == nz - 2:
            send(blk, blk, gc_send, gc_recv, {X: 1 - x, CORE: 1 - c})

    def mean_beside():
        across = ga.at[away + z, c]
        for k, d in enumerate(from_z):
            if abs(d) == 1:
                if k in beside:
                    send(own, own, gz_send, gz_recv.at[k], z_dev(-d))
                send(across, across, gx_send, gx_recv.at[k], z_dev(-d))

    def mean_from_x(i):
        blk = ga.at[away + zof(origins[i]), c]
        came(blk, gx_recv.at[i])
        if origins[i] == 0 and half == 2:
            mean_beside()
        if i != nz - 2:
            send(blk, blk, gc_send, gc_recv, c_nb)

    slot2 = (h * nx + x) * nz + z

    def exchange_squares(condition):
        @pl.when(condition)
        def _():
            with scope("q1"):
                came(all_of(sq1, ny * nc - 1), q_recv.at[0])
                sq2[slot2] = in_pairs([sq1[i] for i in range(ny * nc)])
                for dev in peers2:
                    send(sq2.at[slot2], sq2.at[slot2], q_send.at[1], q_recv.at[1], dev)

    with scope("m_far"):
        momentum_far()
    with scope("ag_x_own"):
        mean_from_x(nz - 1)
    exchange_squares(2 * y >= ny)
    for i in [0, 1] + beyond:
        with scope(f"ag_z{i}"):
            mean_from_z(i)
        if i == 1 and half > 2:
            mean_beside()

    exchange_squares(2 * y < ny)
    for i in [nz - 2] + beside:
        with scope(f"ag_z{i}"):
            mean_from_z(i)
    send(ga.at[column, c], ga.at[column, c], gc_send, gc_col, c_nb)
    with scope("m_x"):
        other = gm.at[pl.ds(away, nz), c]
        came(other, mx_recv)
        send(other, other, mc_send, mc_recv, c_nb)
    with scope("drain1"):
        sent(sib, c_send)
        sent(xs, x_send)
        sent(zr, z_send)
        sent(ar, a_send)
        sent(all_of(xs, nz - 1), gz_send)
        sent(all_of(xs, nz - 1), mz_send)
        sent(all_of(sq1, ny * nc - 1), q_send.at[0])
    for i in [0, 1] + beside:
        with scope(f"ag_x{i}"):
            mean_from_x(i)
    for i in beyond:
        with scope(f"ag_x{i}"):
            mean_from_x(i)

    with scope("m_core"):
        came(gm.at[:, 1 - c], mc_recv)
    with scope("base"):
        load_p.wait()
        for q in range(nq):
            pv[q] = pv[q] - (LR_OUTER * MU_OUTER * MU_OUTER) * gm[q]
    with scope("ag_x_far"):
        mean_from_x(nz - 2)

    with scope("q2"):
        came(all_of(sq2, nh * nq - 1), q_recv.at[1])
        acc = in_pairs([sq2[i] for i in range(nh * nq)])
    with scope("factor"):
        factor = jnp.minimum(1.0, limit * lax.rsqrt(acc + EPSILON))
        at = lambda axis: lax.broadcasted_iota(jnp.int32, (tensors, lanes), axis)
        spread = jnp.sum(jnp.where(at(0) == at(1), factor, 0.0), axis=1, keepdims=True)
        spread = jnp.broadcast_to(spread, (tensors, 128))
        upper = spread.astype(jnp.bfloat16)
        fac[0:tensors, :] = upper
        fac[tensors:lanes, :] = (spread - upper.astype(jnp.float32)).astype(jnp.bfloat16)
        table = fac[...]

    with scope("ag_core"):
        came(ga.at[column, 1 - c], gc_col)
        came(xs, gc_recv)

    with scope("apply"):
        step = 2
        for b in range(0, nq, step):
            spread = jnp.dot(
                hot[pl.ds(b * nc * rows, step * nc * rows), :], table, preferred_element_type=jnp.float32
            ).reshape(step, nc, rows, 128)
            part = pl.ds(b, step)
            newp[part] = pv[part] - (LR_OUTER * (1.0 + MU_OUTER)) * (ga[part] * spread)
        row0 = pl.multiple_of((mine * nc + c) * rows, rows)
        spread = jnp.dot(hot[pl.ds(row0, rows), :], table, preferred_element_type=jnp.float32)
        newm[...] = MU_OUTER * gm[mine, c] + ga[mine, c] * spread

    with scope("drain"):
        sent(xs, gx_send)
        sent(sib, gc_send)
        sent(xs, mx_send)
        sent(sib, mc_send)
        sent(all_of(sq2, nh * nq - 1), q_send.at[1])


def write_out(newp, newm, out_p, out_m, sem):
    copies = [pltpu.make_async_copy(newp, out_p, sem.at[0]), pltpu.make_async_copy(newm, out_m, sem.at[1])]
    for copy in copies:
        copy.start()
    for copy in copies:
        copy.wait()


VMEM_LIMIT = 52 * 1024 * 1024


def on_device(sizes, outer_delta, offsets, parameters, momentum):
    nx, nz, nc, ny, nh = (sizes[a] for a in AXES)
    rows = momentum.shape[0] // 128
    nq = nx * nz
    whole = (nq, nc, rows, 128)
    block = (rows, 128)
    f32 = jnp.float32
    dma = lambda *n: pltpu.SemaphoreType.DMA(n)
    vmem = pltpu.VMEM
    tensors = offsets.shape[0] - 1
    outs = (jax.ShapeDtypeStruct(whole, f32), jax.ShapeDtypeStruct(block, f32))
    in_vmem = (pl.BlockSpec(memory_space=pltpu.VMEM),) * 2
    results = pl.pallas_call(
        functools.partial(step_kernel, sizes),
        out_shape=outs,
        in_specs=[pl.BlockSpec(memory_space=pltpu.HBM)] * 4,
        out_specs=in_vmem,
        scratch_shapes=[
            vmem(whole, f32),
            vmem((nq,) + block, f32),
            vmem((nz,) + block, f32),
            vmem((nz,) + block, f32),
            vmem((nz,) + block, f32),
            vmem((nz - 2,) + block, f32),
            vmem(block, f32),
            vmem(whole, f32),
            vmem(whole, f32),
            vmem(whole, f32),
            vmem((1, tensors + 1), jnp.int32),
            vmem((nq * nc * rows, 2 * tensors), jnp.bfloat16),
            vmem((2 * tensors, 128), jnp.bfloat16),
            vmem((ny * nc, 1, 2 * tensors), f32),
            vmem((nh * nq, 1, 2 * tensors), f32),
            dma(5),
            dma(), dma(nz), dma(),
            dma(), dma(nz),
            dma(), dma(), dma(), dma(),
            dma(), dma(nz - 1), dma(), dma(nz), dma(), dma(), dma(),
            dma(), dma(), dma(), dma(2), dma(), dma(),
            dma(2), dma(2), pltpu.SemaphoreType.REGULAR((nz - 1,)), pltpu.SemaphoreType.REGULAR,
        ],
        compiler_params=pltpu.CompilerParams(
            collective_id=0, has_side_effects=True, vmem_limit_bytes=VMEM_LIMIT
        ),
    )(
        outer_delta.reshape(whole),
        momentum.reshape(block),
        parameters.reshape(whole),
        offsets.reshape(1, tensors + 1),
    )
    new_parameters, new_momentum = pl.pallas_call(
        write_out,
        out_shape=outs,
        in_specs=list(in_vmem),
        out_specs=(pl.BlockSpec(memory_space=pl.ANY),) * 2,
        scratch_shapes=[dma(2)],
        compiler_params=pltpu.CompilerParams(vmem_limit_bytes=4 * 1024 * 1024),
    )(*results)
    return new_parameters.reshape(parameters.shape), new_momentum.reshape(momentum.shape)


def solution(mesh):
    finer = Mesh(mesh.devices.reshape(2, 8, 2, 8, 2), AXES)
    sizes = dict(finer.shape)
    return jax.shard_map(
        functools.partial(on_device, sizes),
        mesh=finer,
        in_specs=(P(REP, SHARD), P(), P(SHARD), P(SHARD_REP)),
        out_specs=(P(SHARD), P(SHARD_REP)),
        check_vma=False,
    )
```
